8 devices in a mesh: data: 8 (over z, y, x, core).
Axes of the slice: x: 2, y: 2, z: 1, core: 2. Of those that a mesh axis runs over, the one named last changes fastest.
Arguments:
- tokens: bfloat16 [16384, 512], P('data')
- d_logits: bfloat16 [16384, 32000], P('data')
- w_up: bfloat16 [2, 512, 1376], replicated
- w_down: bfloat16 [2, 1376, 512], replicated
- w_out: bfloat16 [512, 32000], replicated
- proj_up: bfloat16 [2, 512, 128], replicated
- proj_down: bfloat16 [2, 512, 128], replicated
- mom_up: float32 [2, 128, 1376], P(None, None, 'data')
- var_up: float32 [2, 128, 1376], P(None, None, 'data')
- mom_down: float32 [2, 1376, 128], P(None, 'data')
- var_down: float32 [2, 1376, 128], P(None, 'data')
- mom_out: float32 [512, 32000], P(None, 'data')
- var_out: float32 [512, 32000], P(None, 'data')
Outputs:
- output 1: bfloat16 [2, 512, 1376], replicated
- output 2: bfloat16 [2, 1376, 512], replicated
- output 3: bfloat16 [512, 32000], replicated
- output 4: float32 [2, 128, 1376], P(None, None, 'data')
- output 5: float32 [2, 128, 1376], P(None, None, 'data')
- output 6: float32 [2, 1376, 128], P(None, 'data')
- output 7: float32 [2, 1376, 128], P(None, 'data')
- output 8: float32 [512, 32000], P(None, 'data')
- output 9: float32 [512, 32000], P(None, 'data')
All inputs are finite; a program needn't handle non-finite values.
Results may differ from the reference program's by a relative error of at most 0.00413151.
Values are sent between devices in bfloat16 or wider.
A program may use at most 1 GiB of HBM per device.

```python
import jax
import jax.numpy as jnp

D = 512
FF = 1376
RANK = 128
VOCAB = 32000
TOKENS = 16384
LAYERS = 2
STEP = 4

BETA1 = 0.9
BETA2 = 0.999
EPS = 1e-8
LR = 0.02
ALPHA = 0.5
LR_HEAD = 0.01


def gelu_tanh(values):
    return jax.nn.gelu(values, approximate=True)


def adam_update(gradient, moment_one, moment_two):
    moment_one = BETA1 * moment_one + (1.0 - BETA1) * gradient
    moment_two = BETA2 * moment_two + (1.0 - BETA2) * gradient * gradient
    direction = (moment_one / (1.0 - BETA1 ** STEP)) / (jnp.sqrt(moment_two / (1.0 - BETA2 ** STEP)) + EPS)
    return moment_one, moment_two, direction


def setup_inputs(seed: int = 0) -> dict:
    subkeys = jax.random.split(jax.random.key(seed), 13)
    scale_up = 0.7 * (D / FF) ** 0.5
    scale_down = 0.85
    scale_out = 1.3 * (D / VOCAB) ** 0.5

    def normal(key_num, arr_dims, factor):
        return jax.random.normal(subkeys[key_num], arr_dims, jnp.float32) * factor

    def spread(key_num, arr_dims, factor):
        return jax.random.uniform(subkeys[key_num], arr_dims, jnp.float32, 0.5, 1.5) * factor

    return {
        'tokens': normal(0, (TOKENS, D), 1.0).astype(jnp.bfloat16),
        'd_logits': normal(1, (TOKENS, VOCAB), (D / (VOCAB * TOKENS)) ** 0.5).astype(jnp.bfloat16),
        'w_up': normal(2, (LAYERS, D, FF), D ** -0.5).astype(jnp.bfloat16),
        'w_down': normal(3, (LAYERS, FF, D), FF ** -0.5).astype(jnp.bfloat16),
        'w_out': normal(4, (D, VOCAB), D ** -0.5).astype(jnp.bfloat16),
        'proj_up': normal(5, (LAYERS, D, RANK), D ** -0.5).astype(jnp.bfloat16),
        'proj_down': normal(6, (LAYERS, D, RANK), D ** -0.5).astype(jnp.bfloat16),
        'mom_up': normal(7, (LAYERS, RANK, FF), 0.1 * scale_up),
        'var_up': spread(8, (LAYERS, RANK, FF), 0.003 * scale_up ** 2),
        'mom_down': normal(9, (LAYERS, FF, RANK), 0.1 * scale_down),
        'var_down': spread(10, (LAYERS, FF, RANK), 0.003 * scale_down ** 2),
        'mom_out': normal(11, (D, VOCAB), 0.1 * scale_out),
        'var_out': spread(12, (D, VOCAB), 0.003 * scale_out ** 2),
    }


def layer_forward(hidden, w_first, w_second):
    pre_act = jnp.dot(hidden, w_first, preferred_element_type=jnp.float32).astype(jnp.bfloat16)
    post_act = gelu_tanh(pre_act.astype(jnp.float32)).astype(jnp.bfloat16)
    new_hidden = (hidden.astype(jnp.float32) + jnp.dot(post_act, w_second, preferred_element_type=jnp.float32)).astype(jnp.bfloat16)
    return new_hidden, pre_act, post_act


def reference(tokens, d_logits, w_up, w_down, w_out, proj_up, proj_down, mom_up, var_up, mom_down, var_down, mom_out, var_out):
    hidden = tokens
    saved_acts = []
    for layer_idx in range(LAYERS):
        new_hidden, pre_act, post_act = layer_forward(hidden, w_up[layer_idx], w_down[layer_idx])
        saved_acts.append((hidden, pre_act, post_act))
        hidden = new_hidden
    grad_head = jnp.dot(hidden.T, d_logits, preferred_element_type=jnp.float32)
    grad_hidden = jnp.dot(d_logits, w_out.T, preferred_element_type=jnp.float32).astype(jnp.bfloat16)
    results = []
    for layer_idx in reversed(range(LAYERS)):
        hidden_in, pre_act, post_act = saved_acts[layer_idx]
        grad_down = jnp.dot(post_act.T, grad_hidden, preferred_element_type=jnp.float32)
        d_post = jnp.dot(grad_hidden, w_down[layer_idx].T, preferred_element_type=jnp.float32)
        gelu_pull = jax.vjp(gelu_tanh, pre_act.astype(jnp.float32))[1]
        d_pre = gelu_pull(d_post)[0].astype(jnp.bfloat16)
        grad_up = jnp.dot(hidden_in.T, d_pre, preferred_element_type=jnp.float32)
        if layer_idx > 0:
            grad_hidden = (grad_hidden.astype(jnp.float32) + jnp.dot(d_pre, w_up[layer_idx].T, preferred_element_type=jnp.float32)).astype(jnp.bfloat16)
        low_up = jnp.dot(proj_up[layer_idx].astype(jnp.float32).T, grad_up, preferred_element_type=jnp.float32)
        low_down = jnp.dot(grad_down, proj_down[layer_idx].astype(jnp.float32), preferred_element_type=jnp.float32)
        m_up, v_up, dir_up = adam_update(low_up, mom_up[layer_idx], var_up[layer_idx])
        m_down, v_down, dir_down = adam_update(low_down, mom_down[layer_idx], var_down[layer_idx])
        step_up = jnp.dot(proj_up[layer_idx], dir_up.astype(jnp.bfloat16), preferred_element_type=jnp.float32)
        step_down = jnp.dot(dir_down.astype(jnp.bfloat16), proj_down[layer_idx].T, preferred_element_type=jnp.float32)
        new_up = (w_up[layer_idx].astype(jnp.float32) - LR * ALPHA * step_up).astype(jnp.bfloat16)
        new_down = (w_down[layer_idx].astype(jnp.float32) - LR * ALPHA * step_down).astype(jnp.bfloat16)
        results.append((new_up, new_down, m_up, v_up, m_down, v_down))
    results = results[::-1]
    m_out, v_out, dir_out = adam_update(grad_head, mom_out, var_out)
    w_out_new = (w_out.astype(jnp.float32) - LR_HEAD * dir_out).astype(jnp.bfloat16)
    return (jnp.stack([entry[0] for entry in results]),
            jnp.stack([entry[1] for entry in results]),
            w_out_new,
            jnp.stack([entry[2] for entry in results]),
            jnp.stack([entry[3] for entry in results]),
            jnp.stack([entry[4] for entry in results]),
            jnp.stack([entry[5] for entry in results]),
            m_out,
            v_out)
```

```python
import functools

import jax
import jax.numpy as jnp
from jax import lax
from jax.experimental import pallas as pl
from jax.experimental.pallas import tpu as pltpu
from jax.sharding import PartitionSpec as P

BETA1 = 0.9
BETA2 = 0.999
EPS = 1e-8
STEP = 4
LR = 0.02
ALPHA = 0.5
LR_HEAD = 0.01
DATA_AXIS = 'data'
MESH = pl.DeviceIdType.MESH

BLK = 512
SUBS = 8
SHARD = 4000
RING = 6
DRING = 4

GROUP_DEST = (0, 1, 0, 1, 2, 0, 1, 2, 3, 0, 1, 2, 3, 2, 3, 3)
GROUP_PAIR = (0, 0, 1, 1, 0, 2, 2, 1, 0, 3, 3, 2, 1, 3, 2, 3)
GROUP_SEND = (0, 1, 2, 3, 4, 5, 6, 7, 0, 8, 9, 10, 0, 11, 0, 0)
SENDS = 12
BLOCKS = 64


def lookup(index, values):
    out = jnp.int32(values[-1])
    for position in range(len(values) - 1):
        out = jnp.where(index == position, jnp.int32(values[position]), out)
    return out


def head_kernel(hidden_t, d_logits, w_out,
                grad_t, w_own_t, grad_hidden, recv_core, recv_first, recv_second,
                dz_buf, wo_buf, acc, g_acc, add_core, add_first, add_second, stage, fin, fin_w,
                dz_sem, wo_sem, core_sem, first_sem, second_sem, stage_sem, add_sem, fin_sem, fin_w_sem):
    me = lax.axis_index(DATA_AXIS)
    core = lax.rem(me, 2)
    pos_x = lax.rem(me // 2, 2)
    pos_y = me // 4
    partner = me + 1 - 2 * core
    near_x = me + 2 - 4 * pos_x
    near_y = me + 4 - 8 * pos_y

    barrier = pltpu.get_barrier_semaphore()
    for other in (partner, near_x, near_y):
        pl.semaphore_signal(barrier, inc=1, device_id=(other,), device_id_type=MESH)
    pl.semaphore_wait(barrier, 3)

    def decode(n):
        group = n // 4
        half = lax.rem(n, 2)
        own = lax.rem(n // 2, 2)
        rel = lookup(group, GROUP_DEST)
        far_first = 1 - rel // 2
        far_second = 1 - lax.rem(rel, 2)
        sub = 2 * lookup(group, GROUP_PAIR) + half
        delta_x = jnp.where(half == 0, far_first, far_second)
        delta_y = jnp.where(half == 0, far_second, far_first)
        dest_x = pos_x + delta_x - 2 * pos_x * delta_x
        dest_y = pos_y + delta_y - 2 * pos_y * delta_y
        dest_core = jnp.where(own == 1, core, 1 - core)
        dest = (dest_y * 2 + dest_x) * 2 + dest_core
        col = pl.multiple_of(((125 * dest) // 4 + 4 * sub) * 128, 128)
        return group, half, own, rel, sub, dest, col

    def fetch(n):
        col = decode(n)[-1]
        slot = lax.rem(n, 2)
        return (pltpu.make_async_copy(d_logits.at[:, pl.ds(col, BLK)], dz_buf.at[slot], dz_sem.at[slot]),
                pltpu.make_async_copy(w_out.at[:, pl.ds(col, BLK)], wo_buf.at[slot], wo_sem.at[slot]))

    def send(slot, target_ref, recv_sem, device):
        return pltpu.make_async_remote_copy(
            src_ref=stage.at[slot], dst_ref=target_ref, send_sem=stage_sem.at[slot], recv_sem=recv_sem,
            device_id=(device,), device_id_type=MESH)

    def to_core(slot, index):
        return send(slot, recv_core.at[index], core_sem.at[index], partner)

    def to_first(slot, index, device):
        return send(slot, recv_first.at[index], first_sem.at[index], device)

    def to_second(slot, index, device):
        return send(slot, recv_second.at[index], second_sem.at[index], device)

    def wait_slot(slot):
        to_core(slot, 0).wait_send()

    for copy in fetch(jnp.int32(0)):
        copy.start()
    g_acc[...] = jnp.zeros_like(g_acc)

    def body(n, carry):
        group, half, own, rel, sub, dest, col = decode(n)
        slot = lax.rem(n, 2)

        @pl.when(n + 1 < BLOCKS)
        def _():
            for copy in fetch(n + 1):
                copy.start()

        core_index = sub * 4 + rel
        first_index = sub * 2 + 1 - lax.rem(rel, 2)
        needs_first = jnp.logical_and(own == 1, rel >= 2)
        is_final = jnp.logical_and(own == 1, rel == 3)
        load_core = pltpu.make_async_copy(recv_core.at[core_index], add_core, add_sem.at[0])
        load_first = pltpu.make_async_copy(recv_first.at[first_index], add_first, add_sem.at[1])
        load_second = pltpu.make_async_copy(recv_second.at[sub], add_second, add_sem.at[2])

        for copy in fetch(n):
            copy.wait()

        @pl.loop(0, BLK // 256)
        def _(tile):
            cols = pl.ds(pl.multiple_of(tile * 256, 256), 256)
            acc[:, cols] = jnp.dot(hidden_t[...], dz_buf[slot, :, cols], preferred_element_type=jnp.float32)

        @pl.when(own == 1)
        def _():
            to_core(0, core_index).wait_recv()
            load_core.start()

        @pl.when(needs_first)
        def _():
            to_first(0, first_index, near_x).wait_recv()
            load_first.start()

        @pl.when(is_final)
        def _():
            to_second(0, sub, near_x).wait_recv()
            load_second.start()

        lane = lax.broadcasted_iota(jnp.int32, (1, BLK), 1) + (col - SHARD * dest)
        keep = jnp.where(jnp.logical_and(lane >= 0, lane < SHARD), 1.0, 0.0).astype(jnp.bfloat16)
        weights = wo_buf[slot] * keep

        @pl.loop(0, 4)
        def _(tile):
            rows = pl.ds(pl.multiple_of(tile * 512, 512), 512)
            g_acc[rows, :] += lax.dot_general(dz_buf[slot, rows, :], weights, (((1,), (1,)), ((), ())),
                                              preferred_element_type=jnp.float32)

        @pl.when(own == 0)
        def _():
            place = 2 * RING + lax.rem(group, 2) * 2 + half

            @pl.when(group >= 2)
            def _():
                wait_slot(place)

            stage[place] = acc[...]
            to_core(place, core_index).start()

        turn = lookup(group, GROUP_SEND)
        along_y = jnp.where(rel < 2, half, 1 - half)
        place = along_y * RING + lax.rem(turn, RING)
        device = jnp.where(along_y == 1, near_y, near_x)

        @pl.when(jnp.logical_and(own == 1, rel < 2))
        def _():
            load_core.wait()

            @pl.when(turn >= RING)
            def _():
                wait_slot(place)

            stage[place] = acc[...] + add_core[...]
            to_first(place, first_index, device).start()

        @pl.when(jnp.logical_and(own == 1, rel == 2))
        def _():
            load_core.wait()
            load_first.wait()

            @pl.when(turn >= RING)
            def _():
                wait_slot(place)

            stage[place] = acc[...] + add_core[...] + add_first[...]
            to_second(place, sub, device).start()

        @pl.when(is_final)
        def _():
            load_core.wait()
            load_first.wait()
            load_second.wait()
            rows = pl.ds(pl.multiple_of(sub * BLK, BLK), BLK)
            out_grad = pltpu.make_async_copy(fin.at[half], grad_t.at[rows], fin_sem.at[half])
            out_w = pltpu.make_async_copy(fin_w.at[half], w_own_t.at[rows], fin_w_sem.at[half])

            @pl.when(sub >= 2)
            def _():
                out_grad.wait()
                out_w.wait()

            total = acc[...] + add_core[...] + add_first[...] + add_second[...]
            fin[half] = total.T
            fin_w[half] = wo_buf[slot].T
            out_grad.start()
            out_w.start()

        return carry

    lax.fori_loop(0, BLOCKS, body, 0)

    @pl.loop(0, 4)
    def _(tile):
        rows = pl.ds(pl.multiple_of(tile * 512, 512), 512)
        grad_hidden[rows, :] = g_acc[rows, :].astype(jnp.bfloat16)

    for half in range(2):
        rows = pl.ds((SUBS - 2 + half) * BLK, BLK)
        pltpu.make_async_copy(fin.at[half], grad_t.at[rows], fin_sem.at[half]).wait()
        pltpu.make_async_copy(fin_w.at[half], w_own_t.at[rows], fin_w_sem.at[half]).wait()
    for place in range(2 * RING + DRING):
        wait_slot(place)


def head_gradient(hidden, d_logits, w_out):
    tokens, dim = hidden.shape
    f32 = jnp.float32
    bf16 = jnp.bfloat16
    any_spec = pl.BlockSpec(memory_space=pl.ANY)
    vmem = pl.BlockSpec(memory_space=pltpu.VMEM)
    outs = pl.pallas_call(
        head_kernel,
        out_shape=(
            jax.ShapeDtypeStruct((SUBS * BLK, dim), f32),
            jax.ShapeDtypeStruct((SUBS * BLK, dim), bf16),
            jax.ShapeDtypeStruct((tokens, dim), bf16),
            jax.ShapeDtypeStruct((4 * SUBS, dim, BLK), f32),
            jax.ShapeDtypeStruct((2 * SUBS, dim, BLK), f32),
            jax.ShapeDtypeStruct((SUBS, dim, BLK), f32),
        ),
        in_specs=[vmem, any_spec, any_spec],
        out_specs=(any_spec, any_spec, vmem, any_spec, any_spec, any_spec),
        scratch_shapes=[
            pltpu.VMEM((2, tokens, BLK), bf16),
            pltpu.VMEM((2, dim, BLK), bf16),
            pltpu.VMEM((dim, BLK), f32),
            pltpu.VMEM((tokens, dim), f32),
            pltpu.VMEM((dim, BLK), f32),
            pltpu.VMEM((dim, BLK), f32),
            pltpu.VMEM((dim, BLK), f32),
            pltpu.VMEM((2 * RING + DRING, dim, BLK), f32),
            pltpu.VMEM((2, BLK, dim), f32),
            pltpu.VMEM((2, BLK, dim), bf16),
            pltpu.SemaphoreType.DMA((2,)),
            pltpu.SemaphoreType.DMA((2,)),
            pltpu.SemaphoreType.DMA((4 * SUBS,)),
            pltpu.SemaphoreType.DMA((2 * SUBS,)),
            pltpu.SemaphoreType.DMA((SUBS,)),
            pltpu.SemaphoreType.DMA((2 * RING + DRING,)),
            pltpu.SemaphoreType.DMA((3,)),
            pltpu.SemaphoreType.DMA((2,)),
            pltpu.SemaphoreType.DMA((2,)),
        ],
        compiler_params=pltpu.CompilerParams(collective_id=0, has_side_effects=True, vmem_limit_bytes=56 * 1024 * 1024),
        cost_estimate=pl.CostEstimate(flops=280_000_000_000, bytes_accessed=300_000_000, transcendentals=0),
        name='head_gradient',
    )(hidden.T, d_logits, w_out)
    return outs[0], outs[1], outs[2]


def gelu_tanh(values):
    return jax.nn.gelu(values, approximate=True)


def adam_update(gradient, moment_one, moment_two):
    moment_one = BETA1 * moment_one + (1.0 - BETA1) * gradient
    moment_two = BETA2 * moment_two + (1.0 - BETA2) * gradient * gradient
    direction = (moment_one / (1.0 - BETA1 ** STEP)) / (jnp.sqrt(moment_two / (1.0 - BETA2 ** STEP)) + EPS)
    return moment_one, moment_two, direction


def local_step(tokens, d_logits, w_up, w_down, w_out, proj_up, proj_down, mom_up, var_up, mom_down, var_down, mom_out, var_out):
    num_layers = w_up.shape[0]
    hidden = tokens
    saved_acts = []
    for layer_idx in range(num_layers):
        pre_act = jnp.dot(hidden, w_up[layer_idx], preferred_element_type=jnp.float32).astype(jnp.bfloat16)
        post_act = gelu_tanh(pre_act.astype(jnp.float32)).astype(jnp.bfloat16)
        saved_acts.append((hidden, pre_act, post_act))
        hidden = (hidden.astype(jnp.float32) + jnp.dot(post_act, w_down[layer_idx], preferred_element_type=jnp.float32)).astype(jnp.bfloat16)

    head_window, w_own_window, grad_hidden = head_gradient(hidden, d_logits, w_out)

    me = lax.axis_index(DATA_AXIS)
    offset = 32 * lax.rem(me, 4)
    head_part = lax.dynamic_slice_in_dim(head_window, offset, SHARD, axis=0)
    w_part = lax.dynamic_slice_in_dim(w_own_window, offset, SHARD, axis=0)
    m_out, v_out, dir_out = adam_update(head_part, mom_out.T, var_out.T)
    w_part = (w_part.astype(jnp.float32) - LR_HEAD * dir_out).astype(jnp.bfloat16)
    w_out_new = lax.all_gather(w_part, DATA_AXIS, axis=0, tiled=True).T

    ups = []
    downs = []
    for layer_idx in reversed(range(num_layers)):
        hidden_in, pre_act, post_act = saved_acts[layer_idx]
        grad_down = jnp.einsum('tf,td->fd', post_act, grad_hidden, preferred_element_type=jnp.float32)
        d_post = jnp.einsum('td,fd->tf', grad_hidden, w_down[layer_idx], preferred_element_type=jnp.float32)
        gelu_pull = jax.vjp(gelu_tanh, pre_act.astype(jnp.float32))[1]
        d_pre = gelu_pull(d_post)[0].astype(jnp.bfloat16)
        grad_up = jnp.einsum('tf,td->fd', d_pre, hidden_in, preferred_element_type=jnp.float32)
        if layer_idx > 0:
            grad_hidden = (grad_hidden.astype(jnp.float32) + jnp.einsum('tf,df->td', d_pre, w_up[layer_idx], preferred_element_type=jnp.float32)).astype(jnp.bfloat16)
        low_up = jnp.dot(grad_up, proj_up[layer_idx].astype(jnp.float32), preferred_element_type=jnp.float32)
        low_down = jnp.dot(grad_down, proj_down[layer_idx].astype(jnp.float32), preferred_element_type=jnp.float32)
        ups.append(low_up)
        downs.append(low_down)
    ups = ups[::-1]
    downs = downs[::-1]

    devices = lax.axis_size(DATA_AXIS)
    rank = ups[0].shape[1]
    parts = jnp.stack([low.reshape(devices, -1, rank) for low in ups + downs], axis=1)
    parts = lax.all_to_all(parts, DATA_AXIS, 0, 0, tiled=True)
    sums = jnp.sum(parts, axis=0)
    first = jnp.concatenate([jnp.swapaxes(mom_up, 1, 2), mom_down], axis=0)
    second = jnp.concatenate([jnp.swapaxes(var_up, 1, 2), var_down], axis=0)
    m_low, v_low, dir_low = adam_update(sums, first, second)
    dir_low = dir_low.astype(jnp.bfloat16)

    dir_up = lax.all_gather(dir_low[:num_layers], DATA_AXIS, axis=1, tiled=True)
    dir_down = lax.all_gather(dir_low[num_layers:], DATA_AXIS, axis=1, tiled=True)
    step_up = jnp.einsum('ldr,lfr->ldf', proj_up, dir_up, preferred_element_type=jnp.float32)
    step_down = jnp.einsum('lfr,ldr->lfd', dir_down, proj_down, preferred_element_type=jnp.float32)
    w_up_new = (w_up.astype(jnp.float32) - LR * ALPHA * step_up).astype(jnp.bfloat16)
    w_down_new = (w_down.astype(jnp.float32) - LR * ALPHA * step_down).astype(jnp.bfloat16)

    return (w_up_new, w_down_new, w_out_new,
            jnp.swapaxes(m_low[:num_layers], 1, 2), jnp.swapaxes(v_low[:num_layers], 1, 2),
            m_low[num_layers:], v_low[num_layers:],
            m_out.T, v_out.T)


def solution(mesh):
    row_spec = P(DATA_AXIS, None)
    whole = P()
    up_spec = P(None, None, DATA_AXIS)
    down_spec = P(None, DATA_AXIS, None)
    head_spec = P(None, DATA_AXIS)
    in_specs = (row_spec, row_spec, whole, whole, whole, whole, whole, up_spec, up_spec, down_spec, down_spec, head_spec, head_spec)
    out_specs = (whole, whole, whole, up_spec, up_spec, down_spec, down_spec, head_spec, head_spec)
    return jax.shard_map(local_step, mesh=mesh, in_specs=in_specs, out_specs=out_specs, check_vma=False)
```

```python
import functools

import jax
import jax.numpy as jnp
from jax import lax
from jax.experimental import pallas as pl
from jax.experimental.pallas import tpu as pltpu
from jax.sharding import PartitionSpec as P

BETA1 = 0.9
BETA2 = 0.999
EPS = 1e-8
STEP = 4
LR = 0.02
ALPHA = 0.5
LR_HEAD = 0.01
DATA_AXIS = 'data'
MESH = pl.DeviceIdType.MESH

BLK = 512
SUBS = 8
SHARD = 4000
RING = 6
EDGE = 96
DRING = 4

GROUP_DEST = (0, 1, 0, 1, 2, 0, 1, 2, 3, 0, 1, 2, 3, 2, 3, 3)
GROUP_PAIR = (0, 0, 1, 1, 0, 2, 2, 1, 0, 3, 3, 2, 1, 3, 2, 3)
GROUP_SEND = (0, 1, 2, 3, 4, 5, 6, 7, 0, 8, 9, 10, 0, 11, 0, 0)
SENDS = 12
BLOCKS = 64


def lookup(index, values):
    out = jnp.int32(values[-1])
    for position in range(len(values) - 1):
        out = jnp.where(index == position, jnp.int32(values[position]), out)
    return out


def gelu_tanh(values):
    return jax.nn.gelu(values, approximate=True)


def adam_update(gradient, moment_one, moment_two):
    moment_one = BETA1 * moment_one + (1.0 - BETA1) * gradient
    moment_two = BETA2 * moment_two + (1.0 - BETA2) * gradient * gradient
    direction = (moment_one / (1.0 - BETA1 ** STEP)) / (jnp.sqrt(moment_two / (1.0 - BETA2 ** STEP)) + EPS)
    return moment_one, moment_two, direction


def head_kernel(hidden_t, d_logits, w_out, mom, var, edge,
                w_new, mom_new, var_new, grad_hidden, recv_core, recv_first, recv_second,
                dz_buf, wo_buf, acc, g_acc, add_core, add_first, add_second, stage, moments, fin_w,
                dz_sem, wo_sem, core_sem, first_sem, second_sem, stage_sem, add_sem, load_sem, edge_sem, store_sem, fin_sem):
    me = lax.axis_index(DATA_AXIS)
    core = lax.rem(me, 2)
    pos_x = lax.rem(me // 2, 2)
    pos_y = me // 4
    partner = me + 1 - 2 * core
    near_x = me + 2 - 4 * pos_x
    near_y = me + 4 - 8 * pos_y

    barrier = pltpu.get_barrier_semaphore()
    for other in (partner, near_x, near_y):
        pl.semaphore_signal(barrier, inc=1, device_id=(other,), device_id_type=MESH)
    pl.semaphore_wait(barrier, 3)

    def decode(n):
        group = n // 4
        half = lax.rem(n, 2)
        own = lax.rem(n // 2, 2)
        rel = lookup(group, GROUP_DEST)
        far_first = 1 - rel // 2
        far_second = 1 - lax.rem(rel, 2)
        sub = 2 * lookup(group, GROUP_PAIR) + half
        delta_x = jnp.where(half == 0, far_first, far_second)
        delta_y = jnp.where(half == 0, far_second, far_first)
        dest_x = pos_x + delta_x - 2 * pos_x * delta_x
        dest_y = pos_y + delta_y - 2 * pos_y * delta_y
        dest_core = jnp.where(own == 1, core, 1 - core)
        dest = (dest_y * 2 + dest_x) * 2 + dest_core
        col = pl.multiple_of(((125 * dest) // 4 + 4 * sub) * 128, 128)
        return group, half, own, rel, sub, dest, col

    def fetch(n):
        col = decode(n)[-1]
        slot = lax.rem(n, 2)
        return (pltpu.make_async_copy(d_logits.at[:, pl.ds(col, BLK)], dz_buf.at[slot], dz_sem.at[slot]),
                pltpu.make_async_copy(w_out.at[:, pl.ds(col, BLK)], wo_buf.at[slot], wo_sem.at[slot]))

    def send(slot, target_ref, recv_sem, device):
        return pltpu.make_async_remote_copy(
            src_ref=stage.at[slot], dst_ref=target_ref, send_sem=stage_sem.at[slot], recv_sem=recv_sem,
            device_id=(device,), device_id_type=MESH)

    def to_core(slot, index):
        return send(slot, recv_core.at[index], core_sem.at[index], partner)

    def to_first(slot, index, device):
        return send(slot, recv_first.at[index], first_sem.at[index], device)

    def to_second(slot, index, device):
        return send(slot, recv_second.at[index], second_sem.at[index], device)

    def wait_slot(slot):
        to_core(slot, 0).wait_send()

    shift = 32 * lax.rem(me, 4)

    def moment_loads(sub, half):
        first_row = jnp.clip(BLK * sub - shift, 0, SHARD - BLK)
        place = pl.multiple_of(EDGE + first_row + shift - BLK * sub, 32)
        rows = pl.ds(pl.multiple_of(first_row, 32), BLK)
        return [pltpu.make_async_copy(source.at[rows], moments.at[half, kind, pl.ds(place, BLK)], load_sem.at[half, kind])
                for kind, source in enumerate((mom, var))]

    def edge_loads(half):
        place = pl.ds(pl.multiple_of(BLK + shift, 32), EDGE)
        return [pltpu.make_async_copy(edge.at[kind], moments.at[half, kind, place], edge_sem.at[half, kind])
                for kind in range(2)]

    def moment_stores(sub, half):
        pieces = [(None, EDGE, BLK - 2 * EDGE)]
        for step in range(3):
            pieces.append((jnp.logical_or(sub > 0, 32 * step >= shift), 32 * step, 32))
            pieces.append((jnp.logical_or(sub < SUBS - 1, 32 * step < shift), BLK - EDGE + 32 * step, 32))
        out = []
        for position, (needed, row, size) in enumerate(pieces):
            target = jnp.maximum(BLK * sub - shift + row, 0)
            rows = pl.ds(pl.multiple_of(target, 32), size)
            for kind, result in enumerate((mom_new, var_new)):
                out.append((needed, pltpu.make_async_copy(
                    moments.at[half, kind, pl.ds(EDGE + row, size)], result.at[rows], store_sem.at[half, kind, position])))
        return out

    def weight_store(sub, half):
        cols = pl.ds(pl.multiple_of(sub * BLK, BLK), BLK)
        return pltpu.make_async_copy(fin_w.at[half], w_new.at[:, cols], fin_sem.at[half])

    def for_stores(sub, half, action):
        for needed, copy in moment_stores(sub, half):
            if needed is None:
                action(copy)
            else:
                pl.when(needed)(functools.partial(action, copy))
        action(weight_store(sub, half))

    for copy in fetch(jnp.int32(0)):
        copy.start()
    g_acc[...] = jnp.zeros_like(g_acc)

    def body(n, carry):
        group, half, own, rel, sub, dest, col = decode(n)
        slot = lax.rem(n, 2)

        @pl.when(n + 1 < BLOCKS)
        def _():
            for copy in fetch(n + 1):
                copy.start()

        core_index = sub * 4 + rel
        first_index = sub * 2 + 1 - lax.rem(rel, 2)
        needs_first = jnp.logical_and(own == 1, rel >= 2)
        is_final = jnp.logical_and(own == 1, rel == 3)
        load_core = pltpu.make_async_copy(recv_core.at[core_index], add_core, add_sem.at[0])
        load_first = pltpu.make_async_copy(recv_first.at[first_index], add_first, add_sem.at[1])
        load_second = pltpu.make_async_copy(recv_second.at[sub], add_second, add_sem.at[2])

        for copy in fetch(n):
            copy.wait()

        @pl.loop(0, BLK // 256)
        def _(tile):
            cols = pl.ds(pl.multiple_of(tile * 256, 256), 256)
            acc[:, cols] = jnp.dot(hidden_t[...], dz_buf[slot, :, cols], preferred_element_type=jnp.float32)

        @pl.when(own == 1)
        def _():
            to_core(0, core_index).wait_recv()
            load_core.start()

        @pl.when(needs_first)
        def _():
            to_first(0, first_index, near_x).wait_recv()
            load_first.start()

        @pl.when(is_final)
        def _():
            @pl.when(sub >= 2)
            def _():
                for_stores(sub - 2, half, lambda copy: copy.wait())

            for copy in moment_loads(sub, half):
                copy.start()

            @pl.when(sub == SUBS - 1)
            def _():
                for copy in edge_loads(half):
                    copy.start()

            to_second(0, sub, near_x).wait_recv()
            load_second.start()

        @pl.when(own == 0)
        def _():
            place = 2 * RING + lax.rem(group, 2) * 2 + half

            @pl.when(group >= 2)
            def _():
                wait_slot(place)

            stage[place] = acc[...]
            to_core(place, core_index).start()

        turn = lookup(group, GROUP_SEND)
        along_y = jnp.where(rel < 2, half, 1 - half)
        place = along_y * RING + lax.rem(turn, RING)
        device = jnp.where(along_y == 1, near_y, near_x)

        @pl.when(jnp.logical_and(own == 1, rel < 2))
        def _():
            load_core.wait()

            @pl.when(turn >= RING)
            def _():
                wait_slot(place)

            stage[place] = acc[...] + add_core[...]
            to_first(place, first_index, device).start()

        @pl.when(jnp.logical_and(own == 1, rel == 2))
        def _():
            load_core.wait()
            load_first.wait()

            @pl.when(turn >= RING)
            def _():
                wait_slot(place)

            stage[place] = acc[...] + add_core[...] + add_first[...]
            to_second(place, sub, device).start()

        @pl.when(is_final)
        def _():
            load_core.wait()
            load_first.wait()
            load_second.wait()
            for copy in moment_loads(sub, half):
                copy.wait()

            @pl.when(sub == SUBS - 1)
            def _():
                for copy in edge_loads(half):
                    copy.wait()

            @pl.loop(0, BLK // 128)
            def _(tile):
                cols = pl.ds(pl.multiple_of(tile * 128, 128), 128)
                rows = pl.ds(pl.multiple_of(EDGE + tile * 128, 32), 128)
                total = acc[:, cols] + add_core[:, cols] + add_first[:, cols] + add_second[:, cols]
                first, second, direction = adam_update(total.T, moments[half, 0, rows, :], moments[half, 1, rows, :])
                moments[half, 0, rows, :] = first
                moments[half, 1, rows, :] = second
                fin_w[half, :, cols] = (wo_buf[slot, :, cols].astype(jnp.float32) - LR_HEAD * direction.T).astype(jnp.bfloat16)

            for_stores(sub, half, lambda copy: copy.start())

        lane = lax.broadcasted_iota(jnp.int32, (1, BLK), 1) + (col - SHARD * dest)
        keep = jnp.where(jnp.logical_and(lane >= 0, lane < SHARD), 1.0, 0.0).astype(jnp.bfloat16)
        weights = wo_buf[slot] * keep

        @pl.loop(0, 4)
        def _(tile):
            rows = pl.ds(pl.multiple_of(tile * 512, 512), 512)
            g_acc[rows, :] += lax.dot_general(dz_buf[slot, rows, :], weights, (((1,), (1,)), ((), ())),
                                              preferred_element_type=jnp.float32)

        return carry

    lax.fori_loop(0, BLOCKS, body, 0)

    @pl.loop(0, 4)
    def _(tile):
        rows = pl.ds(pl.multiple_of(tile * 512, 512), 512)
        grad_hidden[rows, :] = g_acc[rows, :].astype(jnp.bfloat16)

    for half in range(2):
        for_stores(SUBS - 2 + half, half, lambda copy: copy.wait())
    for place in range(2 * RING + DRING):
        wait_slot(place)


def head_update(hidden, d_logits, w_out, mom_t, var_t, edge):
    tokens, dim = hidden.shape
    f32 = jnp.float32
    bf16 = jnp.bfloat16
    any_spec = pl.BlockSpec(memory_space=pl.ANY)
    vmem = pl.BlockSpec(memory_space=pltpu.VMEM)
    outs = pl.pallas_call(
        head_kernel,
        out_shape=(
            jax.ShapeDtypeStruct((dim, SUBS * BLK), bf16),
            jax.ShapeDtypeStruct(mom_t.shape, f32),
            jax.ShapeDtypeStruct(var_t.shape, f32),
            jax.ShapeDtypeStruct((tokens, dim), bf16),
            jax.ShapeDtypeStruct((4 * SUBS, dim, BLK), f32),
            jax.ShapeDtypeStruct((2 * SUBS, dim, BLK), f32),
            jax.ShapeDtypeStruct((SUBS, dim, BLK), f32),
        ),
        in_specs=[vmem] + [any_spec] * 5,
        out_specs=(any_spec, any_spec, any_spec, vmem, any_spec, any_spec, any_spec),
        scratch_shapes=[
            pltpu.VMEM((2, tokens, BLK), bf16),
            pltpu.VMEM((2, dim, BLK), bf16),
            pltpu.VMEM((dim, BLK), f32),
            pltpu.VMEM((tokens, dim), f32),
            pltpu.VMEM((dim, BLK), f32),
            pltpu.VMEM((dim, BLK), f32),
            pltpu.VMEM((dim, BLK), f32),
            pltpu.VMEM((2 * RING + DRING, dim, BLK), f32),
            pltpu.VMEM((2, 2, BLK + 2 * EDGE, dim), f32),
            pltpu.VMEM((2, dim, BLK), bf16),
            pltpu.SemaphoreType.DMA((2,)),
            pltpu.SemaphoreType.DMA((2,)),
            pltpu.SemaphoreType.DMA((4 * SUBS,)),
            pltpu.SemaphoreType.DMA((2 * SUBS,)),
            pltpu.SemaphoreType.DMA((SUBS,)),
            pltpu.SemaphoreType.DMA((2 * RING + DRING,)),
            pltpu.SemaphoreType.DMA((3,)),
            pltpu.SemaphoreType.DMA((2, 2)),
            pltpu.SemaphoreType.DMA((2, 2)),
            pltpu.SemaphoreType.DMA((2, 2, 7)),
            pltpu.SemaphoreType.DMA((2,)),
        ],
        compiler_params=pltpu.CompilerParams(collective_id=0, has_side_effects=True, vmem_limit_bytes=56 * 1024 * 1024),
        cost_estimate=pl.CostEstimate(flops=280_000_000_000, bytes_accessed=300_000_000, transcendentals=0),
        name='head_update',
    )(hidden.T, d_logits, w_out, mom_t, var_t, edge)
    return outs[:4]


def local_step(tokens, d_logits, w_up, w_down, w_out, proj_up, proj_down, mom_up, var_up, mom_down, var_down, mom_out, var_out):
    num_layers = w_up.shape[0]
    hidden = tokens
    saved_acts = []
    for layer_idx in range(num_layers):
        pre_act = jnp.dot(hidden, w_up[layer_idx], preferred_element_type=jnp.float32).astype(jnp.bfloat16)
        post_act = gelu_tanh(pre_act.astype(jnp.float32)).astype(jnp.bfloat16)
        saved_acts.append((hidden, pre_act, post_act))
        hidden = (hidden.astype(jnp.float32) + jnp.dot(post_act, w_down[layer_idx], preferred_element_type=jnp.float32)).astype(jnp.bfloat16)

    devices = lax.axis_size(DATA_AXIS)
    mom_t, var_t = mom_out.T, var_out.T
    edge = lax.ppermute(jnp.stack([mom_t[:EDGE], var_t[:EDGE]]), DATA_AXIS, [(dev, dev - 1) for dev in range(1, devices)])
    w_window, m_out, v_out, grad_hidden = head_update(hidden, d_logits, w_out, mom_t, var_t, edge)
    windows = lax.all_gather(w_window, DATA_AXIS, axis=0)
    w_out_new = jnp.concatenate([windows[dev, :, (128 if dev % 4 else 0):] for dev in range(devices)], axis=1)

    ups = []
    downs = []
    for layer_idx in reversed(range(num_layers)):
        hidden_in, pre_act, post_act = saved_acts[layer_idx]
        grad_down = jnp.einsum('tf,td->fd', post_act, grad_hidden, preferred_element_type=jnp.float32)
        d_post = jnp.einsum('td,fd->tf', grad_hidden, w_down[layer_idx], preferred_element_type=jnp.float32)
        gelu_pull = jax.vjp(gelu_tanh, pre_act.astype(jnp.float32))[1]
        d_pre = gelu_pull(d_post)[0].astype(jnp.bfloat16)
        grad_up = jnp.einsum('tf,td->fd', d_pre, hidden_in, preferred_element_type=jnp.float32)
        if layer_idx > 0:
            grad_hidden = (grad_hidden.astype(jnp.float32) + jnp.einsum('tf,df->td', d_pre, w_up[layer_idx], preferred_element_type=jnp.float32)).astype(jnp.bfloat16)
        low_up = jnp.dot(grad_up, proj_up[layer_idx].astype(jnp.float32), preferred_element_type=jnp.float32)
        low_down = jnp.dot(grad_down, proj_down[layer_idx].astype(jnp.float32), preferred_element_type=jnp.float32)
        ups.append(low_up)
        downs.append(low_down)
    ups = ups[::-1]
    downs = downs[::-1]

    rank = ups[0].shape[1]
    parts = jnp.stack([low.reshape(devices, -1, rank) for low in ups + downs], axis=1)
    parts = lax.all_to_all(parts, DATA_AXIS, 0, 0, tiled=True)
    sums = jnp.sum(parts, axis=0)
    first = jnp.concatenate([jnp.swapaxes(mom_up, 1, 2), mom_down], axis=0)
    second = jnp.concatenate([jnp.swapaxes(var_up, 1, 2), var_down], axis=0)
    m_low, v_low, dir_low = adam_update(sums, first, second)
    dir_low = dir_low.astype(jnp.bfloat16)

    dir_up = lax.all_gather(dir_low[:num_layers], DATA_AXIS, axis=1, tiled=True)
    dir_down = lax.all_gather(dir_low[num_layers:], DATA_AXIS, axis=1, tiled=True)
    step_up = jnp.einsum('ldr,lfr->ldf', proj_up, dir_up, preferred_element_type=jnp.float32)
    step_down = jnp.einsum('lfr,ldr->lfd', dir_down, proj_down, preferred_element_type=jnp.float32)
    w_up_new = (w_up.astype(jnp.float32) - LR * ALPHA * step_up).astype(jnp.bfloat16)
    w_down_new = (w_down.astype(jnp.float32) - LR * ALPHA * step_down).astype(jnp.bfloat16)

    return (w_up_new, w_down_new, w_out_new,
            jnp.swapaxes(m_low[:num_layers], 1, 2), jnp.swapaxes(v_low[:num_layers], 1, 2),
            m_low[num_layers:], v_low[num_layers:],
            m_out.T, v_out.T)


def solution(mesh):
    row_spec = P(DATA_AXIS, None)
    whole = P()
    up_spec = P(None, None, DATA_AXIS)
    down_spec = P(None, DATA_AXIS, None)
    head_spec = P(None, DATA_AXIS)
    in_specs = (row_spec, row_spec, whole, whole, whole, whole, whole, up_spec, up_spec, down_spec, down_spec, head_spec, head_spec)
    out_specs = (whole, whole, whole, up_spec, up_spec, down_spec, down_spec, head_spec, head_spec)
    return jax.shard_map(local_step, mesh=mesh, in_specs=in_specs, out_specs=out_specs, check_vma=False)
```

```python
import functools

import jax
import jax.numpy as jnp
from jax import lax
from jax.experimental import pallas as pl
from jax.experimental.pallas import tpu as pltpu
from jax.sharding import PartitionSpec as P

BETA1 = 0.9
BETA2 = 0.999
EPS = 1e-8
STEP = 4
LR = 0.02
ALPHA = 0.5
LR_HEAD = 0.01
DATA_AXIS = 'data'
MESH = pl.DeviceIdType.MESH

BLK = 512
SUBS = 8
SHARD = 4000
RING = 6
EDGE = 96
DRING = 4

GROUP_DEST = (0, 1, 0, 1, 2, 0, 1, 2, 3, 0, 1, 2, 3, 2, 3, 3)
GROUP_PAIR = (0, 0, 1, 1, 0, 2, 2, 1, 0, 3, 3, 2, 1, 3, 2, 3)
GROUP_SEND = (0, 1, 2, 3, 4, 5, 6, 7, 0, 8, 9, 10, 0, 11, 0, 0)
SENDS = 12
BLOCKS = 64


def lookup(index, values):
    out = jnp.int32(values[-1])
    for position in range(len(values) - 1):
        out = jnp.where(index == position, jnp.int32(values[position]), out)
    return out


def gelu_tanh(values):
    return jax.nn.gelu(values, approximate=True)


def adam_update(gradient, moment_one, moment_two):
    moment_one = BETA1 * moment_one + (1.0 - BETA1) * gradient
    moment_two = BETA2 * moment_two + (1.0 - BETA2) * gradient * gradient
    direction = (moment_one / (1.0 - BETA1 ** STEP)) / (jnp.sqrt(moment_two / (1.0 - BETA2 ** STEP)) + EPS)
    return moment_one, moment_two, direction


def head_kernel(hidden_t, d_logits, w_out, mom, var, edge,
                w_new, mom_new, var_new, grad_hidden, recv_core, recv_first, recv_second,
                dz_buf, wo_buf, acc, g_acc, add_core, add_first, add_second, stage, moments, fin_w,
                dz_sem, wo_sem, core_sem, first_sem, second_sem, stage_sem, add_sem, load_sem, edge_sem, store_sem, fin_sem):
    me = lax.axis_index(DATA_AXIS)
    core = lax.rem(me, 2)
    pos_x = lax.rem(me // 2, 2)
    pos_y = me // 4
    partner = me + 1 - 2 * core
    near_x = me + 2 - 4 * pos_x
    near_y = me + 4 - 8 * pos_y

    barrier = pltpu.get_barrier_semaphore()
    for other in (partner, near_x, near_y):
        pl.semaphore_signal(barrier, inc=1, device_id=(other,), device_id_type=MESH)
    pl.semaphore_wait(barrier, 3)

    def decode(n):
        group = n // 4
        half = lax.rem(n, 2)
        own = lax.rem(n // 2, 2)
        rel = lookup(group, GROUP_DEST)
        far_first = 1 - rel // 2
        far_second = 1 - lax.rem(rel, 2)
        sub = 2 * lookup(group, GROUP_PAIR) + half
        delta_x = jnp.where(half == 0, far_first, far_second)
        delta_y = jnp.where(half == 0, far_second, far_first)
        dest_x = pos_x + delta_x - 2 * pos_x * delta_x
        dest_y = pos_y + delta_y - 2 * pos_y * delta_y
        dest_core = jnp.where(own == 1, core, 1 - core)
        dest = (dest_y * 2 + dest_x) * 2 + dest_core
        col = pl.multiple_of(((125 * dest) // 4 + 4 * sub) * 128, 128)
        return group, half, own, rel, sub, dest, col

    def fetch(n):
        col = decode(n)[-1]
        slot = lax.rem(n, 2)
        return (pltpu.make_async_copy(d_logits.at[:, pl.ds(col, BLK)], dz_buf.at[slot], dz_sem.at[slot]),
                pltpu.make_async_copy(w_out.at[:, pl.ds(col, BLK)], wo_buf.at[slot], wo_sem.at[slot]))

    def send(slot, target_ref, recv_sem, device):
        return pltpu.make_async_remote_copy(
            src_ref=stage.at[slot], dst_ref=target_ref, send_sem=stage_sem.at[slot], recv_sem=recv_sem,
            device_id=(device,), device_id_type=MESH)

    def to_core(slot, index):
        return send(slot, recv_core.at[index], core_sem.at[index], partner)

    def to_first(slot, index, device):
        return send(slot, recv_first.at[index], first_sem.at[index], device)

    def to_second(slot, index, device):
        return send(slot, recv_second.at[index], second_sem.at[index], device)

    def wait_slot(slot):
        to_core(slot, 0).wait_send()

    shift = 32 * lax.rem(me, 4)

    def moment_loads(sub, half):
        first_row = jnp.clip(BLK * sub - shift, 0, SHARD - BLK)
        place = pl.multiple_of(EDGE + first_row + shift - BLK * sub, 32)
        rows = pl.ds(pl.multiple_of(first_row, 32), BLK)
        return [pltpu.make_async_copy(source.at[rows], moments.at[half, kind, pl.ds(place, BLK)], load_sem.at[half, kind])
                for kind, source in enumerate((mom, var))]

    def edge_loads(half):
        place = pl.ds(pl.multiple_of(BLK + shift, 32), EDGE)
        return [pltpu.make_async_copy(edge.at[kind], moments.at[half, kind, place], edge_sem.at[half, kind])
                for kind in range(2)]

    def moment_stores(sub, half):
        pieces = [(None, EDGE, BLK - 2 * EDGE)]
        for step in range(3):
            pieces.append((jnp.logical_or(sub > 0, 32 * step >= shift), 32 * step, 32))
            pieces.append((jnp.logical_or(sub < SUBS - 1, 32 * step < shift), BLK - EDGE + 32 * step, 32))
        out = []
        for position, (needed, row, size) in enumerate(pieces):
            target = jnp.maximum(BLK * sub - shift + row, 0)
            rows = pl.ds(pl.multiple_of(target, 32), size)
            for kind, result in enumerate((mom_new, var_new)):
                out.append((needed, pltpu.make_async_copy(
                    moments.at[half, kind, pl.ds(EDGE + row, size)], result.at[rows], store_sem.at[half, kind, position])))
        return out

    def weight_store(sub, half):
        cols = pl.ds(pl.multiple_of(lax.rem(sub, SUBS // 2) * BLK, BLK), BLK)
        return pltpu.make_async_copy(fin_w.at[half], w_new.at[sub // (SUBS // 2), :, cols], fin_sem.at[half])

    def for_stores(sub, half, action):
        for needed, copy in moment_stores(sub, half):
            if needed is None:
                action(copy)
            else:
                pl.when(needed)(functools.partial(action, copy))
        action(weight_store(sub, half))

    for copy in fetch(jnp.int32(0)):
        copy.start()
    g_acc[...] = jnp.zeros_like(g_acc)

    def body(n, carry):
        group, half, own, rel, sub, dest, col = decode(n)
        slot = lax.rem(n, 2)

        @pl.when(n + 1 < BLOCKS)
        def _():
            for copy in fetch(n + 1):
                copy.start()

        core_index = sub * 4 + rel
        first_index = sub * 2 + 1 - lax.rem(rel, 2)
        needs_first = jnp.logical_and(own == 1, rel >= 2)
        is_final = jnp.logical_and(own == 1, rel == 3)
        load_core = pltpu.make_async_copy(recv_core.at[core_index], add_core, add_sem.at[0])
        load_first = pltpu.make_async_copy(recv_first.at[first_index], add_first, add_sem.at[1])
        load_second = pltpu.make_async_copy(recv_second.at[sub], add_second, add_sem.at[2])

        for copy in fetch(n):
            copy.wait()

        @pl.loop(0, BLK // 256)
        def _(tile):
            cols = pl.ds(pl.multiple_of(tile * 256, 256), 256)
            acc[:, cols] = jnp.dot(hidden_t[...], dz_buf[slot, :, cols], preferred_element_type=jnp.float32)

        @pl.when(own == 1)
        def _():
            to_core(0, core_index).wait_recv()
            load_core.start()

        @pl.when(needs_first)
        def _():
            to_first(0, first_index, near_x).wait_recv()
            load_first.start()

        @pl.when(is_final)
        def _():
            @pl.when(sub >= 2)
            def _():
                for_stores(sub - 2, half, lambda copy: copy.wait())

            for copy in moment_loads(sub, half):
                copy.start()

            @pl.when(sub == SUBS - 1)
            def _():
                for copy in edge_loads(half):
                    copy.start()

        @pl.when(own == 0)
        def _():
            place = 2 * RING + lax.rem(group, 2) * 2 + half

            @pl.when(group >= 2)
            def _():
                wait_slot(place)

            stage[place] = acc[...]
            to_core(place, core_index).start()

        turn = lookup(group, GROUP_SEND)
        along_y = jnp.where(rel < 2, half, 1 - half)
        place = along_y * RING + lax.rem(turn, RING)
        device = jnp.where(along_y == 1, near_y, near_x)

        @pl.when(jnp.logical_and(own == 1, rel < 2))
        def _():
            load_core.wait()

            @pl.when(turn >= RING)
            def _():
                wait_slot(place)

            stage[place] = acc[...] + add_core[...]
            to_first(place, first_index, device).start()

        @pl.when(jnp.logical_and(own == 1, rel == 2))
        def _():
            load_core.wait()
            load_first.wait()

            @pl.when(turn >= RING)
            def _():
                wait_slot(place)

            stage[place] = acc[...] + add_core[...] + add_first[...]
            to_second(place, sub, device).start()

        lane = lax.broadcasted_iota(jnp.int32, (1, BLK), 1) + (col - SHARD * dest)
        keep = jnp.where(jnp.logical_and(lane >= 0, lane < SHARD), 1.0, 0.0).astype(jnp.bfloat16)
        weights = wo_buf[slot] * keep

        @pl.loop(0, 4)
        def _(tile):
            rows = pl.ds(pl.multiple_of(tile * 512, 512), 512)
            g_acc[rows, :] += lax.dot_general(dz_buf[slot, rows, :], weights, (((1,), (1,)), ((), ())),
                                              preferred_element_type=jnp.float32)

        @pl.when(is_final)
        def _():
            to_second(0, sub, near_x).wait_recv()
            load_second.start()
            load_core.wait()
            load_first.wait()
            load_second.wait()
            for copy in moment_loads(sub, half):
                copy.wait()

            @pl.when(sub == SUBS - 1)
            def _():
                for copy in edge_loads(half):
                    copy.wait()

            @pl.loop(0, BLK // 128)
            def _(tile):
                cols = pl.ds(pl.multiple_of(tile * 128, 128), 128)
                rows = pl.ds(pl.multiple_of(EDGE + tile * 128, 32), 128)
                total = acc[:, cols] + add_core[:, cols] + add_first[:, cols] + add_second[:, cols]
                first, second, direction = adam_update(total.T, moments[half, 0, rows, :], moments[half, 1, rows, :])
                moments[half, 0, rows, :] = first
                moments[half, 1, rows, :] = second
                fin_w[half, :, cols] = (wo_buf[slot, :, cols].astype(jnp.float32) - LR_HEAD * direction.T).astype(jnp.bfloat16)

            for_stores(sub, half, lambda copy: copy.start())

        return carry

    lax.fori_loop(0, BLOCKS, body, 0)

    @pl.loop(0, 4)
    def _(tile):
        rows = pl.ds(pl.multiple_of(tile * 512, 512), 512)
        grad_hidden[rows, :] = g_acc[rows, :].astype(jnp.bfloat16)

    for half in range(2):
        for_stores(SUBS - 2 + half, half, lambda copy: copy.wait())
    for place in range(2 * RING + DRING):
        wait_slot(place)


def head_update(hidden, d_logits, w_out, mom_t, var_t, edge):
    tokens, dim = hidden.shape
    f32 = jnp.float32
    bf16 = jnp.bfloat16
    any_spec = pl.BlockSpec(memory_space=pl.ANY)
    vmem = pl.BlockSpec(memory_space=pltpu.VMEM)
    outs = pl.pallas_call(
        head_kernel,
        out_shape=(
            jax.ShapeDtypeStruct((2, dim, SUBS * BLK // 2), bf16),
            jax.ShapeDtypeStruct(mom_t.shape, f32),
            jax.ShapeDtypeStruct(var_t.shape, f32),
            jax.ShapeDtypeStruct((tokens, dim), bf16),
            jax.ShapeDtypeStruct((4 * SUBS, dim, BLK), f32),
            jax.ShapeDtypeStruct((2 * SUBS, dim, BLK), f32),
            jax.ShapeDtypeStruct((SUBS, dim, BLK), f32),
        ),
        in_specs=[vmem] + [any_spec] * 5,
        out_specs=(any_spec, any_spec, any_spec, vmem, any_spec, any_spec, any_spec),
        scratch_shapes=[
            pltpu.VMEM((2, tokens, BLK), bf16),
            pltpu.VMEM((2, dim, BLK), bf16),
            pltpu.VMEM((dim, BLK), f32),
            pltpu.VMEM((tokens, dim), f32),
            pltpu.VMEM((dim, BLK), f32),
            pltpu.VMEM((dim, BLK), f32),
            pltpu.VMEM((dim, BLK), f32),
            pltpu.VMEM((2 * RING + DRING, dim, BLK), f32),
            pltpu.VMEM((2, 2, BLK + 2 * EDGE, dim), f32),
            pltpu.VMEM((2, dim, BLK), bf16),
            pltpu.SemaphoreType.DMA((2,)),
            pltpu.SemaphoreType.DMA((2,)),
            pltpu.SemaphoreType.DMA((4 * SUBS,)),
            pltpu.SemaphoreType.DMA((2 * SUBS,)),
            pltpu.SemaphoreType.DMA((SUBS,)),
            pltpu.SemaphoreType.DMA((2 * RING + DRING,)),
            pltpu.SemaphoreType.DMA((3,)),
            pltpu.SemaphoreType.DMA((2, 2)),
            pltpu.SemaphoreType.DMA((2, 2)),
            pltpu.SemaphoreType.DMA((2, 2, 7)),
            pltpu.SemaphoreType.DMA((2,)),
        ],
        compiler_params=pltpu.CompilerParams(collective_id=0, has_side_effects=True, vmem_limit_bytes=56 * 1024 * 1024),
        cost_estimate=pl.CostEstimate(flops=280_000_000_000, bytes_accessed=300_000_000, transcendentals=0),
        name='head_update',
    )(hidden.T, d_logits, w_out, mom_t, var_t, edge)
    return outs[:4]


def flip(me, far):
    for bit, weight in zip(far, (2, 4, 1)):
        if bit:
            me = me + weight - 2 * weight * lax.rem(me // weight, 2)
    return me


def permute(value, far):
    mask = 2 * far[0] + 4 * far[1] + far[2]
    return lax.ppermute(value, DATA_AXIS, [(dev, dev ^ mask) for dev in range(8)])


def place_kernel(origins, num_copies, has_base, *refs):
    count = len(origins)
    pieces = refs[:count]
    sources = refs[count:count + num_copies]
    refs = refs[count + num_copies + has_base:]
    out, targets = refs[0], refs[1:1 + num_copies]
    buf, in_sem, out_sem, edge_sem = refs[1 + num_copies:5 + num_copies]
    me = lax.axis_index(DATA_AXIS)
    width = pieces[0].shape[-1]
    loads = [pltpu.make_async_copy(piece, buf.at[position], in_sem.at[position]) for position, piece in enumerate(pieces)]
    for load in loads:
        load.start()
    if num_copies:
        wide, wide_in, wide_out = refs[5 + num_copies:]
        rows = wide.shape[1]
        steps = sources[0].shape[0] // rows
        work = [(kind, step) for step in range(steps) for kind in range(num_copies)]

        def wide_load(index):
            kind, step = work[index]
            return pltpu.make_async_copy(sources[kind].at[pl.ds(step * rows, rows)], wide.at[index % 4], wide_in.at[index % 4])

        def wide_store(index):
            kind, step = work[index]
            return pltpu.make_async_copy(wide.at[index % 4], targets[kind].at[pl.ds(step * rows, rows)], wide_out.at[index % 4])

        for index in range(2):
            wide_load(index).start()
        for index in range(len(work)):
            wide_load(index).wait()
            wide_store(index).start()
            if index + 2 < len(work):
                if index >= 2:
                    wide_store(index - 2).wait()
                wide_load(index + 2).start()
        for index in range(len(work) - 4, len(work)):
            wide_store(index).wait()
    stores = []
    for position, (far, part) in enumerate(origins):
        loads[position].wait()
        dest = flip(me, far)
        col = pl.multiple_of(((125 * dest) // 4) * 128 + part * width, 128)
        skip = 0 if part else 128
        store = pltpu.make_async_copy(buf.at[position, :, pl.ds(skip, width - skip)],
                                      out.at[:, pl.ds(pl.multiple_of(col + skip, 128), width - skip)], out_sem.at[position])
        store.start()
        stores.append(store)
        if not part:
            edge = pltpu.make_async_copy(buf.at[position, :, pl.ds(0, 128)], out.at[:, pl.ds(col, 128)], edge_sem.at[position])

            @pl.when(lax.rem(dest, 4) == 0)
            def _():
                edge.start()
                edge.wait()
    for store in stores:
        store.wait()


def place(base, placed, vocab, copies=()):
    pieces = [piece for piece, _, _ in placed]
    origins = tuple((far, part) for _, far, part in placed)
    dim, width = pieces[0].shape
    count = len(pieces)
    has_base = base is not None
    args = pieces + list(copies) + ([base] if has_base else [])
    scratch = [pltpu.VMEM((count, dim, width), jnp.bfloat16)] + [pltpu.SemaphoreType.DMA((count,))] * 3
    if copies:
        scratch += [pltpu.VMEM((4, 400, dim), jnp.float32), pltpu.SemaphoreType.DMA((4,)), pltpu.SemaphoreType.DMA((4,))]
    any_spec = pl.BlockSpec(memory_space=pl.ANY)
    outs = pl.pallas_call(
        functools.partial(place_kernel, origins, len(copies), int(has_base)),
        out_shape=[jax.ShapeDtypeStruct((dim, vocab), jnp.bfloat16)] + [jax.ShapeDtypeStruct(c.shape, c.dtype) for c in copies],
        in_specs=[any_spec] * len(args),
        out_specs=[any_spec] * (1 + len(copies)),
        scratch_shapes=scratch,
        input_output_aliases={len(args) - 1: 0} if has_base else {},
        compiler_params=pltpu.CompilerParams(vmem_limit_bytes=40 * 1024 * 1024),
        cost_estimate=pl.CostEstimate(flops=6_000_000_000 if copies else 3_000_000_000, bytes_accessed=count * 4 * dim * width, transcendentals=0),
        name='place',
    )(*args)
    return outs


NEAR = ((1, 0), (0, 1), (1, 1))


def small_kernel(parts, mom, var, mom_new, var_new, dirs, from_core, from_chip, stage,
                 core_send, core_recv, chip_send, chip_recv, gather_send, gather_recv, back_send, back_recv):
    me = lax.axis_index(DATA_AXIS)
    partner = flip(me, (0, 0, 1))
    chips = [me] + [flip(me, far + (0,)) for far in NEAR]
    barrier = pltpu.get_barrier_semaphore()
    for other in chips[1:] + [partner]:
        pl.semaphore_signal(barrier, inc=1, device_id=(other,), device_id_type=MESH)
    pl.semaphore_wait(barrier, 4)

    def remote(source, target, send_sem, recv_sem, device):
        return pltpu.make_async_remote_copy(src_ref=source, dst_ref=target, send_sem=send_sem, recv_sem=recv_sem,
                                            device_id=(device,), device_id_type=MESH)

    order = (1, 2, 3, 0)
    to_core = {}
    for k in order:
        to_core[k] = remote(parts.at[flip(chips[k], (0, 0, 1))], from_core.at[k], core_send.at[k], core_recv.at[k], partner)
        to_core[k].start()
    to_chip = []
    for k in (1, 2, 3):
        to_core[k].wait_recv()
        stage[k - 1] = parts[chips[k]] + from_core[k]
        copy = remote(stage.at[k - 1], from_chip.at[k - 1], chip_send.at[k - 1], chip_recv.at[k - 1], chips[k])
        copy.start()
        to_chip.append(copy)
    to_core[0].wait_recv()
    for copy in to_chip:
        copy.wait_recv()
    total = parts[me] + from_core[0] + from_chip[0] + from_chip[1] + from_chip[2]
    first, second, direction = adam_update(total, mom[...], var[...])
    mom_new[...] = first
    var_new[...] = second
    dirs[me] = direction.astype(jnp.bfloat16)
    gather = [remote(dirs.at[me], dirs.at[me], gather_send.at[k - 1], gather_recv.at[k - 1], chips[k]) for k in (1, 2, 3)]
    back = [remote(dirs.at[chips[k]], dirs.at[chips[k]], back_send.at[k], back_recv.at[k], partner) for k in range(4)]
    for copy in gather:
        copy.start()
    back[0].start()
    for k in (1, 2, 3):
        remote(dirs.at[chips[k]], dirs.at[chips[k]], gather_send.at[k - 1], gather_recv.at[k - 1], chips[k]).wait_recv()
        back[k].start()
    for k in range(4):
        remote(dirs.at[flip(chips[k], (0, 0, 1))], dirs.at[flip(chips[k], (0, 0, 1))], back_send.at[k], back_recv.at[k], partner).wait_recv()
        back[k].wait_send()
        to_core[k].wait_send()
    for copy in gather + to_chip:
        copy.wait_send()


def small_update(parts, mom, var):
    shape = parts.shape[1:]
    f32 = jnp.float32
    vmem = pl.BlockSpec(memory_space=pltpu.VMEM)
    dma = pltpu.SemaphoreType.DMA
    return pl.pallas_call(
        small_kernel,
        out_shape=(jax.ShapeDtypeStruct(shape, f32), jax.ShapeDtypeStruct(shape, f32),
                   jax.ShapeDtypeStruct(parts.shape, jnp.bfloat16)),
        in_specs=[vmem] * 3,
        out_specs=(vmem,) * 3,
        scratch_shapes=[pltpu.VMEM((4,) + shape, f32), pltpu.VMEM((3,) + shape, f32), pltpu.VMEM((3,) + shape, f32),
                        dma((4,)), dma((4,)), dma((3,)), dma((3,)), dma((3,)), dma((3,)), dma((4,)), dma((4,))],
        compiler_params=pltpu.CompilerParams(collective_id=1, has_side_effects=True, vmem_limit_bytes=32 * 1024 * 1024),
        cost_estimate=pl.CostEstimate(flops=30_000_000_000, bytes_accessed=10_000_000, transcendentals=0),
        name='small_update',
    )(parts, mom, var)


def local_step(tokens, d_logits, w_up, w_down, w_out, proj_up, proj_down, mom_up, var_up, mom_down, var_down, mom_out, var_out):
    num_layers = w_up.shape[0]
    hidden = tokens
    saved_acts = []
    for layer_idx in range(num_layers):
        pre_act = jnp.dot(hidden, w_up[layer_idx], preferred_element_type=jnp.float32).astype(jnp.bfloat16)
        post_act = gelu_tanh(pre_act.astype(jnp.float32)).astype(jnp.bfloat16)
        saved_acts.append((hidden, pre_act, post_act))
        hidden = (hidden.astype(jnp.float32) + jnp.dot(post_act, w_down[layer_idx], preferred_element_type=jnp.float32)).astype(jnp.bfloat16)

    devices = lax.axis_size(DATA_AXIS)
    mom_t, var_t = mom_out.T, var_out.T
    edge = lax.ppermute(jnp.stack([mom_t[:EDGE], var_t[:EDGE]]), DATA_AXIS, [(dev, dev - 1) for dev in range(1, devices)])
    w_window, m_raw, v_raw, grad_hidden = head_update(hidden, d_logits, w_out, mom_t, var_t, edge)
    left, right = w_window[0], w_window[1]
    far_x, far_y, far_xy, near = (1, 0, 0), (0, 1, 0), (1, 1, 0), (0, 0, 0)
    left_x = permute(left, far_x)
    right_y = permute(right, far_y)
    left_y = permute(left, far_y)
    right_x = permute(right, far_x)

    def with_core(pieces):
        return pieces + [(permute(piece, (0, 0, 1)), (far[0], far[1], 1), part) for piece, far, part in pieces]

    ups = []
    downs = []
    for layer_idx in reversed(range(num_layers)):
        hidden_in, pre_act, post_act = saved_acts[layer_idx]
        grad_down = jnp.einsum('tf,td->fd', post_act, grad_hidden, preferred_element_type=jnp.float32)
        d_post = jnp.einsum('td,fd->tf', grad_hidden, w_down[layer_idx], preferred_element_type=jnp.float32)
        gelu_pull = jax.vjp(gelu_tanh, pre_act.astype(jnp.float32))[1]
        d_pre = gelu_pull(d_post)[0].astype(jnp.bfloat16)
        grad_up = jnp.einsum('tf,td->fd', d_pre, hidden_in, preferred_element_type=jnp.float32)
        if layer_idx > 0:
            grad_hidden = (grad_hidden.astype(jnp.float32) + jnp.einsum('tf,df->td', d_pre, w_up[layer_idx], preferred_element_type=jnp.float32)).astype(jnp.bfloat16)
        low_up = jnp.dot(grad_up, proj_up[layer_idx].astype(jnp.float32), preferred_element_type=jnp.float32)
        low_down = jnp.dot(grad_down, proj_down[layer_idx].astype(jnp.float32), preferred_element_type=jnp.float32)
        ups.append(low_up)
        downs.append(low_down)
        if layer_idx == num_layers - 1:
            grad_hidden, left_x, right_y = lax.optimization_barrier((grad_hidden, left_x, right_y))
            left_xy = permute(left_x, far_y)
            right_xy = permute(right_y, far_x)
    ups = ups[::-1]
    downs = downs[::-1]

    vocab = d_logits.shape[1]
    w_new, m_out, v_out = place(None, with_core([(left, near, 0), (right, near, 1)]), vocab, (m_raw, v_raw))
    w_new, = place(w_new, with_core([(left_x, far_x, 0), (right_y, far_y, 1)]), vocab)

    rank = ups[0].shape[1]
    parts = jnp.stack([low.reshape(devices, -1, rank) for low in ups + downs], axis=1)
    first = jnp.concatenate([jnp.swapaxes(mom_up, 1, 2), mom_down], axis=0)
    second = jnp.concatenate([jnp.swapaxes(var_up, 1, 2), var_down], axis=0)
    w_new, parts = lax.optimization_barrier((w_new, parts))
    m_low, v_low, dirs = small_update(parts, first, second)
    m_low, left_xy, right_xy = lax.optimization_barrier((m_low, left_xy, right_xy))
    dirs = jnp.swapaxes(dirs, 0, 1).reshape(2 * num_layers, -1, rank)
    step_up = jnp.einsum('ldr,lfr->ldf', proj_up, dirs[:num_layers], preferred_element_type=jnp.float32)
    step_down = jnp.einsum('lfr,ldr->lfd', dirs[num_layers:], proj_down, preferred_element_type=jnp.float32)
    w_up_new = (w_up.astype(jnp.float32) - LR * ALPHA * step_up).astype(jnp.bfloat16)
    w_down_new = (w_down.astype(jnp.float32) - LR * ALPHA * step_down).astype(jnp.bfloat16)

    w_new, = place(w_new, with_core([(left_y, far_y, 0), (right_x, far_x, 1)]), vocab)
    w_out_new, = place(w_new, with_core([(left_xy, far_xy, 0), (right_xy, far_xy, 1)]), vocab)

    return (w_up_new, w_down_new, w_out_new,
            jnp.swapaxes(m_low[:num_layers], 1, 2), jnp.swapaxes(v_low[:num_layers], 1, 2),
            m_low[num_layers:], v_low[num_layers:],
            m_out.T, v_out.T)


def solution(mesh):
    row_spec = P(DATA_AXIS, None)
    whole = P()
    up_spec = P(None, None, DATA_AXIS)
    down_spec = P(None, DATA_AXIS, None)
    head_spec = P(None, DATA_AXIS)
    in_specs = (row_spec, row_spec, whole, whole, whole, whole, whole, up_spec, up_spec, down_spec, down_spec, head_spec, head_spec)
    out_specs = (whole, whole, whole, up_spec, up_spec, down_spec, down_spec, head_spec, head_spec)
    return jax.shard_map(local_step, mesh=mesh, in_specs=in_specs, out_specs=out_specs, check_vma=False)
```

```python
import functools

import jax
import jax.numpy as jnp
from jax import lax
from jax.experimental import pallas as pl
from jax.experimental.pallas import tpu as pltpu
from jax.sharding import PartitionSpec as P

BETA1 = 0.9
BETA2 = 0.999
EPS = 1e-8
STEP = 4
LR = 0.02
ALPHA = 0.5
LR_HEAD = 0.01
DATA_AXIS = 'data'
MESH = pl.DeviceIdType.MESH

BLK = 512
SUBS = 8
SHARD = 4000
RING = 6
EDGE = 96
DRING = 4

GROUP_DEST = (0, 1, 0, 1, 2, 0, 1, 2, 3, 0, 1, 2, 3, 2, 3, 3)
GROUP_PAIR = (0, 0, 1, 1, 0, 2, 2, 1, 0, 3, 3, 2, 1, 3, 2, 3)
GROUP_SEND = (0, 1, 2, 3, 4, 5, 6, 7, 0, 8, 9, 10, 0, 11, 0, 0)
SENDS = 12
BLOCKS = 64


def lookup(index, values):
    out = jnp.int32(values[-1])
    for position in range(len(values) - 1):
        out = jnp.where(index == position, jnp.int32(values[position]), out)
    return out


def gelu_tanh(values):
    return jax.nn.gelu(values, approximate=True)


def adam_update(gradient, moment_one, moment_two):
    moment_one = BETA1 * moment_one + (1.0 - BETA1) * gradient
    moment_two = BETA2 * moment_two + (1.0 - BETA2) * gradient * gradient
    direction = (moment_one / (1.0 - BETA1 ** STEP)) / (jnp.sqrt(moment_two / (1.0 - BETA2 ** STEP)) + EPS)
    return moment_one, moment_two, direction


def head_kernel(hidden_t, d_logits, w_out, mom, var, edge,
                w_left, w_right, mom_new, var_new, grad_hidden, recv_core, recv_first,
                dz_buf, wo_buf, acc, g_acc, add_core, add_first, recv_second, stage, moments, fin_w,
                dz_sem, wo_sem, core_sem, first_sem, second_sem, stage_sem, add_sem, load_sem, edge_sem, store_sem, fin_sem):
    me = lax.axis_index(DATA_AXIS)
    core = lax.rem(me, 2)
    pos_x = lax.rem(me // 2, 2)
    pos_y = me // 4
    partner = me + 1 - 2 * core
    near_x = me + 2 - 4 * pos_x
    near_y = me + 4 - 8 * pos_y

    barrier = pltpu.get_barrier_semaphore()
    for other in (partner, near_x, near_y):
        pl.semaphore_signal(barrier, inc=1, device_id=(other,), device_id_type=MESH)
    pl.semaphore_wait(barrier, 3)

    def decode(n):
        group = n // 4
        half = lax.rem(n, 2)
        own = lax.rem(n // 2, 2)
        rel = lookup(group, GROUP_DEST)
        far_first = 1 - rel // 2
        far_second = 1 - lax.rem(rel, 2)
        sub = 2 * lookup(group, GROUP_PAIR) + half
        delta_x = jnp.where(half == 0, far_first, far_second)
        delta_y = jnp.where(half == 0, far_second, far_first)
        dest_x = pos_x + delta_x - 2 * pos_x * delta_x
        dest_y = pos_y + delta_y - 2 * pos_y * delta_y
        dest_core = jnp.where(own == 1, core, 1 - core)
        dest = (dest_y * 2 + dest_x) * 2 + dest_core
        col = pl.multiple_of(((125 * dest) // 4 + 4 * sub) * 128, 128)
        return group, half, own, rel, sub, dest, col

    def fetch(n):
        col = decode(n)[-1]
        slot = lax.rem(n, 2)
        return (pltpu.make_async_copy(d_logits.at[:, pl.ds(col, BLK)], dz_buf.at[slot], dz_sem.at[slot]),
                pltpu.make_async_copy(w_out.at[:, pl.ds(col, BLK)], wo_buf.at[slot], wo_sem.at[slot]))

    def send(slot, target_ref, recv_sem, device):
        return pltpu.make_async_remote_copy(
            src_ref=stage.at[slot], dst_ref=target_ref, send_sem=stage_sem.at[slot], recv_sem=recv_sem,
            device_id=(device,), device_id_type=MESH)

    def to_core(slot, index):
        return send(slot, recv_core.at[index], core_sem.at[index], partner)

    def to_first(slot, index, device):
        return send(slot, recv_first.at[index], first_sem.at[index], device)

    def to_second(slot, index, device):
        return send(slot, recv_second.at[index], second_sem.at[index], device)

    def wait_slot(slot):
        to_core(slot, 0).wait_send()

    shift = 32 * lax.rem(me, 4)

    def moment_loads(sub, half):
        first_row = jnp.clip(BLK * sub - shift, 0, SHARD - BLK)
        place = pl.multiple_of(EDGE + first_row + shift - BLK * sub, 32)
        rows = pl.ds(pl.multiple_of(first_row, 32), BLK)
        return [pltpu.make_async_copy(source.at[rows], moments.at[half, kind, pl.ds(place, BLK)], load_sem.at[half, kind])
                for kind, source in enumerate((mom, var))]

    def edge_loads(half):
        place = pl.ds(pl.multiple_of(BLK + shift, 32), EDGE)
        return [pltpu.make_async_copy(edge.at[kind], moments.at[half, kind, place], edge_sem.at[half, kind])
                for kind in range(2)]

    def moment_stores(sub, half):
        pieces = [(None, EDGE, BLK - 2 * EDGE)]
        for step in range(3):
            pieces.append((jnp.logical_or(sub > 0, 32 * step >= shift), 32 * step, 32))
            pieces.append((jnp.logical_or(sub < SUBS - 1, 32 * step < shift), BLK - EDGE + 32 * step, 32))
        out = []
        for position, (needed, row, size) in enumerate(pieces):
            target = jnp.maximum(BLK * sub - shift + row, 0)
            rows = pl.ds(pl.multiple_of(target, 32), size)
            for kind, result in enumerate((mom_new, var_new)):
                out.append((needed, pltpu.make_async_copy(
                    moments.at[half, kind, pl.ds(EDGE + row, size)], result.at[rows], store_sem.at[half, kind, position])))
        return out

    def weight_stores(sub, half):
        cols = pl.ds(pl.multiple_of(lax.rem(sub, SUBS // 2) * BLK, BLK), BLK)
        return [(sub < SUBS // 2, pltpu.make_async_copy(fin_w.at[half], w_left.at[:, cols], fin_sem.at[half])),
                (sub >= SUBS // 2, pltpu.make_async_copy(fin_w.at[half], w_right.at[:, cols], fin_sem.at[half]))]

    def for_stores(sub, half, action):
        for needed, copy in moment_stores(sub, half) + weight_stores(sub, half):
            if needed is None:
                action(copy)
            else:
                pl.when(needed)(functools.partial(action, copy))

    for copy in fetch(jnp.int32(0)):
        copy.start()
    g_acc[...] = jnp.zeros_like(g_acc)

    def body(n, carry):
        group, half, own, rel, sub, dest, col = decode(n)
        slot = lax.rem(n, 2)

        @pl.when(n + 1 < BLOCKS)
        def _():
            for copy in fetch(n + 1):
                copy.start()

        core_index = sub * 4 + rel
        first_index = sub * 2 + 1 - lax.rem(rel, 2)
        needs_first = jnp.logical_and(own == 1, rel >= 2)
        is_final = jnp.logical_and(own == 1, rel == 3)
        load_core = pltpu.make_async_copy(recv_core.at[core_index], add_core.at[half], add_sem.at[half, 0])
        load_first = pltpu.make_async_copy(recv_first.at[first_index], add_first.at[half], add_sem.at[half, 1])

        for copy in fetch(n):
            copy.wait()

        @pl.loop(0, BLK // 256)
        def _(tile):
            cols = pl.ds(pl.multiple_of(tile * 256, 256), 256)
            acc[half, :, cols] = jnp.dot(hidden_t[...], dz_buf[slot, :, cols], preferred_element_type=jnp.float32)

        @pl.when(own == 1)
        def _():
            to_core(0, core_index).wait_recv()
            load_core.start()

        @pl.when(needs_first)
        def _():
            to_first(0, first_index, near_x).wait_recv()
            load_first.start()

        @pl.when(is_final)
        def _():
            @pl.when(sub >= 2)
            def _():
                for_stores(sub - 2, half, lambda copy: copy.wait())

            for copy in moment_loads(sub, half):
                copy.start()

            @pl.when(sub == SUBS - 1)
            def _():
                for copy in edge_loads(half):
                    copy.start()

            fin_w[half] = wo_buf[slot]

        @pl.when(own == 0)
        def _():
            place = 2 * RING + lax.rem(group, 2) * 2 + half

            @pl.when(group >= 2)
            def _():
                wait_slot(place)

            stage[place] = acc[half]
            to_core(place, core_index).start()

        turn = lookup(group, GROUP_SEND)
        along_y = jnp.where(rel < 2, half, 1 - half)
        place = along_y * RING + lax.rem(turn, RING)
        device = jnp.where(along_y == 1, near_y, near_x)

        @pl.when(jnp.logical_and(own == 1, rel < 2))
        def _():
            load_core.wait()

            @pl.when(turn >= RING)
            def _():
                wait_slot(place)

            stage[place] = acc[half] + add_core[half]
            to_first(place, first_index, device).start()

        @pl.when(jnp.logical_and(own == 1, rel == 2))
        def _():
            load_core.wait()
            load_first.wait()

            @pl.when(turn >= RING)
            def _():
                wait_slot(place)

            stage[place] = acc[half] + add_core[half] + add_first[half]
            to_second(place, sub, device).start()

        lane = lax.broadcasted_iota(jnp.int32, (1, BLK), 1) + (col - SHARD * dest)
        keep = jnp.where(jnp.logical_and(lane >= 0, lane < SHARD), 1.0, 0.0).astype(jnp.bfloat16)
        weights = wo_buf[slot] * keep

        @pl.loop(0, 4)
        def _(tile):
            rows = pl.ds(pl.multiple_of(tile * 512, 512), 512)
            g_acc[rows, :] += lax.dot_general(dz_buf[slot, rows, :], weights, (((1,), (1,)), ((), ())),
                                              preferred_element_type=jnp.float32)

        @pl.when(jnp.logical_and(is_final, half == 1))
        def _():
            for part in range(2):
                this = sub - 1 + part
                to_second(0, this, near_x).wait_recv()
                pltpu.make_async_copy(recv_core.at[this * 4 + 3], add_core.at[part], add_sem.at[part, 0]).wait()
                pltpu.make_async_copy(recv_first.at[this * 2], add_first.at[part], add_sem.at[part, 1]).wait()
                for copy in moment_loads(this, part):
                    copy.wait()

                @pl.when(this == SUBS - 1)
                def _():
                    for copy in edge_loads(part):
                        copy.wait()

            @pl.loop(0, 2 * (BLK // 128))
            def _(tile):
                part = tile // (BLK // 128)
                tile = lax.rem(tile, BLK // 128)
                cols = pl.ds(pl.multiple_of(tile * 128, 128), 128)
                rows = pl.ds(pl.multiple_of(EDGE + tile * 128, 32), 128)
                total = acc[part, :, cols] + add_core[part, :, cols] + add_first[part, :, cols] + recv_second[sub - 1 + part, :, cols]
                first, second, direction = adam_update(total.T, moments[part, 0, rows, :], moments[part, 1, rows, :])
                moments[part, 0, rows, :] = first
                moments[part, 1, rows, :] = second
                fin_w[part, :, cols] = (fin_w[part, :, cols].astype(jnp.float32) - LR_HEAD * direction.T).astype(jnp.bfloat16)

            for part in range(2):
                for_stores(sub - 1 + part, part, lambda copy: copy.start())

        return carry

    lax.fori_loop(0, BLOCKS, body, 0)

    @pl.loop(0, 4)
    def _(tile):
        rows = pl.ds(pl.multiple_of(tile * 512, 512), 512)
        grad_hidden[rows, :] = g_acc[rows, :].astype(jnp.bfloat16)

    for half in range(2):
        for_stores(SUBS - 2 + half, half, lambda copy: copy.wait())
    for place in range(2 * RING + DRING):
        wait_slot(place)


def head_update(hidden, d_logits, w_out, mom_t, var_t, edge):
    tokens, dim = hidden.shape
    f32 = jnp.float32
    bf16 = jnp.bfloat16
    any_spec = pl.BlockSpec(memory_space=pl.ANY)
    vmem = pl.BlockSpec(memory_space=pltpu.VMEM)
    outs = pl.pallas_call(
        head_kernel,
        out_shape=(
            jax.ShapeDtypeStruct((dim, SUBS * BLK // 2), bf16),
            jax.ShapeDtypeStruct((dim, SUBS * BLK // 2), bf16),
            jax.ShapeDtypeStruct(mom_t.shape, f32),
            jax.ShapeDtypeStruct(var_t.shape, f32),
            jax.ShapeDtypeStruct((tokens, dim), bf16),
            jax.ShapeDtypeStruct((4 * SUBS, dim, BLK), f32),
            jax.ShapeDtypeStruct((2 * SUBS, dim, BLK), f32),
        ),
        in_specs=[vmem] + [any_spec] * 5,
        out_specs=(any_spec, any_spec, any_spec, any_spec, vmem, any_spec, any_spec),
        scratch_shapes=[
            pltpu.VMEM((2, tokens, BLK), bf16),
            pltpu.VMEM((2, dim, BLK), bf16),
            pltpu.VMEM((2, dim, BLK), f32),
            pltpu.VMEM((tokens, dim), f32),
            pltpu.VMEM((2, dim, BLK), f32),
            pltpu.VMEM((2, dim, BLK), f32),
            pltpu.VMEM((SUBS, dim, BLK), f32),
            pltpu.VMEM((2 * RING + DRING, dim, BLK), f32),
            pltpu.VMEM((2, 2, BLK + 2 * EDGE, dim), f32),
            pltpu.VMEM((2, dim, BLK), bf16),
            pltpu.SemaphoreType.DMA((2,)),
            pltpu.SemaphoreType.DMA((2,)),
            pltpu.SemaphoreType.DMA((4 * SUBS,)),
            pltpu.SemaphoreType.DMA((2 * SUBS,)),
            pltpu.SemaphoreType.DMA((SUBS,)),
            pltpu.SemaphoreType.DMA((2 * RING + DRING,)),
            pltpu.SemaphoreType.DMA((2, 2)),
            pltpu.SemaphoreType.DMA((2, 2)),
            pltpu.SemaphoreType.DMA((2, 2)),
            pltpu.SemaphoreType.DMA((2, 2, 7)),
            pltpu.SemaphoreType.DMA((2,)),
        ],
        compiler_params=pltpu.CompilerParams(collective_id=0, has_side_effects=True, vmem_limit_bytes=56 * 1024 * 1024),
        cost_estimate=pl.CostEstimate(flops=280_000_000_000, bytes_accessed=300_000_000, transcendentals=0),
        name='head_update',
    )(hidden.T, d_logits, w_out, mom_t, var_t, edge)
    return outs[:5]


def flip(me, far):
    for bit, weight in zip(far, (2, 4, 1)):
        if bit:
            me = me + weight - 2 * weight * lax.rem(me // weight, 2)
    return me


def permute(value, far):
    mask = 2 * far[0] + 4 * far[1] + far[2]
    return lax.ppermute(value, DATA_AXIS, [(dev, dev ^ mask) for dev in range(8)])


def place_kernel(origins, num_copies, has_base, *refs):
    count = len(origins)
    pieces = refs[:count]
    sources = refs[count:count + num_copies]
    refs = refs[count + num_copies + has_base:]
    out, targets = refs[0], refs[1:1 + num_copies]
    buf, in_sem, out_sem, edge_sem = refs[1 + num_copies:5 + num_copies]
    me = lax.axis_index(DATA_AXIS)
    width = pieces[0].shape[-1]
    loads = [pltpu.make_async_copy(piece, buf.at[position], in_sem.at[position]) for position, piece in enumerate(pieces)]
    for load in loads:
        load.start()
    if num_copies:
        wide, wide_in, wide_out = refs[5 + num_copies:]
        rows = wide.shape[1]
        steps = sources[0].shape[0] // rows
        work = [(kind, step) for step in range(steps) for kind in range(num_copies)]

        def wide_load(index):
            kind, step = work[index]
            return pltpu.make_async_copy(sources[kind].at[pl.ds(step * rows, rows)], wide.at[index % 4], wide_in.at[index % 4])

        def wide_store(index):
            kind, step = work[index]
            return pltpu.make_async_copy(wide.at[index % 4], targets[kind].at[pl.ds(step * rows, rows)], wide_out.at[index % 4])

        for index in range(2):
            wide_load(index).start()
        for index in range(len(work)):
            wide_load(index).wait()
            wide_store(index).start()
            if index + 2 < len(work):
                if index >= 2:
                    wide_store(index - 2).wait()
                wide_load(index + 2).start()
        for index in range(len(work) - 4, len(work)):
            wide_store(index).wait()
    stores = []
    for position, (far, part) in enumerate(origins):
        loads[position].wait()
        dest = flip(me, far)
        col = pl.multiple_of(((125 * dest) // 4) * 128 + part * width, 128)
        skip = 0 if part else 128
        store = pltpu.make_async_copy(buf.at[position, :, pl.ds(skip, width - skip)],
                                      out.at[:, pl.ds(pl.multiple_of(col + skip, 128), width - skip)], out_sem.at[position])
        store.start()
        stores.append(store)
        if not part:
            edge = pltpu.make_async_copy(buf.at[position, :, pl.ds(0, 128)], out.at[:, pl.ds(col, 128)], edge_sem.at[position])

            @pl.when(lax.rem(dest, 4) == 0)
            def _():
                edge.start()
                edge.wait()
    for store in stores:
        store.wait()


def place(base, placed, vocab, copies=()):
    pieces = [piece for piece, _, _ in placed]
    origins = tuple((far, part) for _, far, part in placed)
    dim, width = pieces[0].shape
    count = len(pieces)
    has_base = base is not None
    args = pieces + list(copies) + ([base] if has_base else [])
    scratch = [pltpu.VMEM((count, dim, width), jnp.bfloat16)] + [pltpu.SemaphoreType.DMA((count,))] * 3
    if copies:
        scratch += [pltpu.VMEM((4, 400, dim), jnp.float32), pltpu.SemaphoreType.DMA((4,)), pltpu.SemaphoreType.DMA((4,))]
    any_spec = pl.BlockSpec(memory_space=pl.ANY)
    outs = pl.pallas_call(
        functools.partial(place_kernel, origins, len(copies), int(has_base)),
        out_shape=[jax.ShapeDtypeStruct((dim, vocab), jnp.bfloat16)] + [jax.ShapeDtypeStruct(c.shape, c.dtype) for c in copies],
        in_specs=[any_spec] * len(args),
        out_specs=[any_spec] * (1 + len(copies)),
        scratch_shapes=scratch,
        input_output_aliases={len(args) - 1: 0} if has_base else {},
        compiler_params=pltpu.CompilerParams(vmem_limit_bytes=40 * 1024 * 1024),
        cost_estimate=pl.CostEstimate(flops=6_000_000_000 if copies else 3_000_000_000, bytes_accessed=count * 4 * dim * width, transcendentals=0),
        name='place',
    )(*args)
    return outs


NEAR = ((1, 0), (0, 1), (1, 1))


def small_kernel(up_0, up_1, down_0, down_1, mom, var, mom_new, var_new, dir_up, dir_down,
                 parts, dirs, whole, from_core, from_chip, stage,
                 core_send, core_recv, chip_send, chip_recv, gather_send, gather_recv, back_send, back_recv):
    me = lax.axis_index(DATA_AXIS)
    partner = flip(me, (0, 0, 1))
    chips = [me] + [flip(me, far + (0,)) for far in NEAR]
    barrier = pltpu.get_barrier_semaphore()
    for other in chips[1:] + [partner]:
        pl.semaphore_signal(barrier, inc=1, device_id=(other,), device_id_type=MESH)
    pl.semaphore_wait(barrier, 4)

    shard = parts.shape[2]
    lows = (up_0, up_1, down_0, down_1)
    for dev in range(parts.shape[0]):
        for kind, low in enumerate(lows):
            parts[dev, kind] = low[dev * shard:(dev + 1) * shard, :]

    def remote(source, target, send_sem, recv_sem, device):
        return pltpu.make_async_remote_copy(src_ref=source, dst_ref=target, send_sem=send_sem, recv_sem=recv_sem,
                                            device_id=(device,), device_id_type=MESH)

    order = (1, 2, 3, 0)
    to_core = {}
    for k in order:
        to_core[k] = remote(parts.at[flip(chips[k], (0, 0, 1))], from_core.at[k], core_send.at[k], core_recv.at[k], partner)
        to_core[k].start()
    to_chip = []
    for k in (1, 2, 3):
        to_core[k].wait_recv()
        stage[k - 1] = parts[chips[k]] + from_core[k]
        copy = remote(stage.at[k - 1], from_chip.at[k - 1], chip_send.at[k - 1], chip_recv.at[k - 1], chips[k])
        copy.start()
        to_chip.append(copy)
    to_core[0].wait_recv()
    for copy in to_chip:
        copy.wait_recv()
    total = parts[me] + from_core[0] + from_chip[0] + from_chip[1] + from_chip[2]
    first, second, direction = adam_update(total, mom[...], var[...])
    mom_new[...] = first
    var_new[...] = second
    dirs[me] = direction.astype(jnp.bfloat16)
    gather = [remote(dirs.at[me], dirs.at[me], gather_send.at[k - 1], gather_recv.at[k - 1], chips[k]) for k in (1, 2, 3)]
    back = [remote(dirs.at[chips[k]], dirs.at[chips[k]], back_send.at[k], back_recv.at[k], partner) for k in range(4)]
    for copy in gather:
        copy.start()
    back[0].start()
    for k in (1, 2, 3):
        remote(dirs.at[chips[k]], dirs.at[chips[k]], gather_send.at[k - 1], gather_recv.at[k - 1], chips[k]).wait_recv()
        back[k].start()
    for k in range(4):
        remote(dirs.at[flip(chips[k], (0, 0, 1))], dirs.at[flip(chips[k], (0, 0, 1))], back_send.at[k], back_recv.at[k], partner).wait_recv()
        back[k].wait_send()
        to_core[k].wait_send()
    for copy in gather + to_chip:
        copy.wait_send()
    for kind in range(4):
        for dev in range(parts.shape[0]):
            whole[dev * shard:(dev + 1) * shard, :] = dirs[dev, kind].astype(jnp.float32)
        target = dir_up if kind < 2 else dir_down
        target[kind % 2] = whole[...].astype(jnp.bfloat16)


def small_update(lows, mom, var):
    shape = mom.shape
    rows, rank = lows[0].shape
    devices = rows // shape[1]
    f32 = jnp.float32
    vmem = pl.BlockSpec(memory_space=pltpu.VMEM)
    dma = pltpu.SemaphoreType.DMA
    return pl.pallas_call(
        small_kernel,
        out_shape=(jax.ShapeDtypeStruct(shape, f32), jax.ShapeDtypeStruct(shape, f32),
                   jax.ShapeDtypeStruct((2, rows, rank), jnp.bfloat16), jax.ShapeDtypeStruct((2, rows, rank), jnp.bfloat16)),
        in_specs=[vmem] * 6,
        out_specs=(vmem,) * 4,
        scratch_shapes=[pltpu.VMEM((devices,) + shape, f32), pltpu.VMEM((devices,) + shape, jnp.bfloat16),
                        pltpu.VMEM((rows, rank), f32), pltpu.VMEM((4,) + shape, f32), pltpu.VMEM((3,) + shape, f32), pltpu.VMEM((3,) + shape, f32),
                        dma((4,)), dma((4,)), dma((3,)), dma((3,)), dma((3,)), dma((3,)), dma((4,)), dma((4,))],
        compiler_params=pltpu.CompilerParams(collective_id=1, has_side_effects=True, vmem_limit_bytes=32 * 1024 * 1024),
        cost_estimate=pl.CostEstimate(flops=30_000_000_000, bytes_accessed=10_000_000, transcendentals=0),
        name='small_update',
    )(*lows, mom, var)


def local_step(tokens, d_logits, w_up, w_down, w_out, proj_up, proj_down, mom_up, var_up, mom_down, var_down, mom_out, var_out):
    num_layers = w_up.shape[0]
    hidden = tokens
    saved_acts = []
    for layer_idx in range(num_layers):
        pre_act = jnp.dot(hidden, w_up[layer_idx], preferred_element_type=jnp.float32).astype(jnp.bfloat16)
        post_act = gelu_tanh(pre_act.astype(jnp.float32)).astype(jnp.bfloat16)
        saved_acts.append((hidden, pre_act, post_act))
        hidden = (hidden.astype(jnp.float32) + jnp.dot(post_act, w_down[layer_idx], preferred_element_type=jnp.float32)).astype(jnp.bfloat16)

    devices = lax.axis_size(DATA_AXIS)
    mom_t, var_t = mom_out.T, var_out.T
    edge = lax.ppermute(jnp.stack([mom_t[:EDGE], var_t[:EDGE]]), DATA_AXIS, [(dev, dev - 1) for dev in range(1, devices)])
    left, right, m_raw, v_raw, grad_hidden = head_update(hidden, d_logits, w_out, mom_t, var_t, edge)
    far_x, far_y, far_xy, near = (1, 0, 0), (0, 1, 0), (1, 1, 0), (0, 0, 0)
    left_x = permute(left, far_x)
    right_y = permute(right, far_y)
    left_y = permute(left, far_y)
    right_x = permute(right, far_x)

    def with_core(pieces):
        return pieces + [(permute(piece, (0, 0, 1)), (far[0], far[1], 1), part) for piece, far, part in pieces]

    ups = []
    downs = []
    for layer_idx in reversed(range(num_layers)):
        hidden_in, pre_act, post_act = saved_acts[layer_idx]
        grad_down = jnp.einsum('tf,td->fd', post_act, grad_hidden, preferred_element_type=jnp.float32)
        d_post = jnp.einsum('td,fd->tf', grad_hidden, w_down[layer_idx], preferred_element_type=jnp.float32)
        gelu_pull = jax.vjp(gelu_tanh, pre_act.astype(jnp.float32))[1]
        d_pre = gelu_pull(d_post)[0].astype(jnp.bfloat16)
        grad_up = jnp.einsum('tf,td->fd', d_pre, hidden_in, preferred_element_type=jnp.float32)
        if layer_idx > 0:
            grad_hidden = (grad_hidden.astype(jnp.float32) + jnp.einsum('tf,df->td', d_pre, w_up[layer_idx], preferred_element_type=jnp.float32)).astype(jnp.bfloat16)
        low_up = jnp.dot(grad_up, proj_up[layer_idx].astype(jnp.float32), preferred_element_type=jnp.float32)
        low_down = jnp.dot(grad_down, proj_down[layer_idx].astype(jnp.float32), preferred_element_type=jnp.float32)
        ups.append(low_up)
        downs.append(low_down)
        if layer_idx == num_layers - 1:
            grad_hidden, left_x, right_y = lax.optimization_barrier((grad_hidden, left_x, right_y))
            left_xy = permute(left_x, far_y)
            right_xy = permute(right_y, far_x)
    ups = ups[::-1]
    downs = downs[::-1]

    vocab = d_logits.shape[1]
    ups[0], left_y, right_x = lax.optimization_barrier((ups[0], left_y, right_x))
    w_new, m_out, v_out = place(None, with_core([(left, near, 0), (right, near, 1)]), vocab, (m_raw, v_raw))
    w_new, = place(w_new, with_core([(left_x, far_x, 0), (right_y, far_y, 1)]), vocab)

    w_new, = place(w_new, with_core([(left_y, far_y, 0), (right_x, far_x, 1)]), vocab)
    first = jnp.concatenate([jnp.swapaxes(mom_up, 1, 2), mom_down], axis=0)
    second = jnp.concatenate([jnp.swapaxes(var_up, 1, 2), var_down], axis=0)
    lows = ups + downs
    w_new, lows[0] = lax.optimization_barrier((w_new, lows[0]))
    m_low, v_low, dir_up, dir_down = small_update(lows, first, second)
    m_low, left_xy, right_xy = lax.optimization_barrier((m_low, left_xy, right_xy))
    step_up = jnp.einsum('ldr,lfr->ldf', proj_up, dir_up, preferred_element_type=jnp.float32)
    step_down = jnp.einsum('lfr,ldr->lfd', dir_down, proj_down, preferred_element_type=jnp.float32)
    w_up_new = (w_up.astype(jnp.float32) - LR * ALPHA * step_up).astype(jnp.bfloat16)
    w_down_new = (w_down.astype(jnp.float32) - LR * ALPHA * step_down).astype(jnp.bfloat16)

    w_out_new, = place(w_new, with_core([(left_xy, far_xy, 0), (right_xy, far_xy, 1)]), vocab)

    return (w_up_new, w_down_new, w_out_new,
            jnp.swapaxes(m_low[:num_layers], 1, 2), jnp.swapaxes(v_low[:num_layers], 1, 2),
            m_low[num_layers:], v_low[num_layers:],
            m_out.T, v_out.T)


def solution(mesh):
    row_spec = P(DATA_AXIS, None)
    whole = P()
    up_spec = P(None, None, DATA_AXIS)
    down_spec = P(None, DATA_AXIS, None)
    head_spec = P(None, DATA_AXIS)
    in_specs = (row_spec, row_spec, whole, whole, whole, whole, whole, up_spec, up_spec, down_spec, down_spec, head_spec, head_spec)
    out_specs = (whole, whole, whole, up_spec, up_spec, down_spec, down_spec, head_spec, head_spec)
    return jax.shard_map(local_step, mesh=mesh, in_specs=in_specs, out_specs=out_specs, check_vma=False)
```

```python
import functools

import jax
import jax.numpy as jnp
from jax import lax
from jax.experimental import pallas as pl
from jax.experimental.pallas import tpu as pltpu
from jax.sharding import PartitionSpec as P


BETA1 = 0.9
BETA2 = 0.999
EPS = 1e-8
STEP = 4
LR = 0.02
ALPHA = 0.5
LR_HEAD = 0.01
DATA_AXIS = 'data'
MESH = pl.DeviceIdType.MESH

BLK = 512
SUBS = 8
SHARD = 4000
RING = 6
EDGE = 96
DRING = 4

GROUP_DEST = (0, 1, 0, 1, 2, 0, 1, 2, 3, 0, 1, 2, 3, 2, 3, 3)
GROUP_PAIR = (0, 0, 1, 1, 0, 2, 2, 1, 0, 3, 3, 2, 1, 3, 2, 3)
GROUP_SEND = (0, 1, 2, 3, 4, 5, 6, 7, 0, 8, 9, 10, 0, 11, 0, 0)
BLOCKS = 64


def lookup(index, values):
    out = jnp.int32(values[-1])
    for position in range(len(values) - 1):
        out = jnp.where(index == position, jnp.int32(values[position]), out)
    return out


def gelu_tanh(values):
    return jax.nn.gelu(values, approximate=True)


def adam_update(gradient, moment_one, moment_two):
    moment_one = BETA1 * moment_one + (1.0 - BETA1) * gradient
    moment_two = BETA2 * moment_two + (1.0 - BETA2) * gradient * gradient
    direction = (moment_one / (1.0 - BETA1 ** STEP)) / (jnp.sqrt(moment_two / (1.0 - BETA2 ** STEP)) + EPS)
    return moment_one, moment_two, direction


def head_kernel(hidden_t, d_logits, w_out, mom, var, edge,
                w_left, w_right, mom_new, var_new, grad_hidden, recv_core, recv_first,
                dz_buf, wo_buf, acc, g_acc, add_core, add_first, recv_second, stage, moments, fin_w,
                dz_sem, wo_sem, core_sem, first_sem, second_sem, stage_sem, add_sem, load_sem, edge_sem, store_sem, fin_sem):
    me = lax.axis_index(DATA_AXIS)
    core = lax.rem(me, 2)
    pos_x = lax.rem(me // 2, 2)
    pos_y = me // 4
    partner = me + 1 - 2 * core
    near_x = me + 2 - 4 * pos_x
    near_y = me + 4 - 8 * pos_y

    barrier = pltpu.get_barrier_semaphore()
    for other in (partner, near_x, near_y):
        pl.semaphore_signal(barrier, inc=1, device_id=(other,), device_id_type=MESH)
    pl.semaphore_wait(barrier, 3)

    def decode(n):
        group = n // 4
        half = lax.rem(n, 2)
        own = lax.rem(n // 2, 2)
        rel = lookup(group, GROUP_DEST)
        far_first = 1 - rel // 2
        far_second = 1 - lax.rem(rel, 2)
        sub = 2 * lookup(group, GROUP_PAIR) + half
        delta_x = jnp.where(half == 0, far_first, far_second)
        delta_y = jnp.where(half == 0, far_second, far_first)
        dest_x = pos_x + delta_x - 2 * pos_x * delta_x
        dest_y = pos_y + delta_y - 2 * pos_y * delta_y
        dest_core = jnp.where(own == 1, core, 1 - core)
        dest = (dest_y * 2 + dest_x) * 2 + dest_core
        col = pl.multiple_of(((125 * dest) // 4 + 4 * sub) * 128, 128)
        return group, half, own, rel, sub, dest, col

    def fetch(n):
        col = decode(n)[-1]
        slot = lax.rem(n, 2)
        return (pltpu.make_async_copy(d_logits.at[:, pl.ds(col, BLK)], dz_buf.at[slot], dz_sem.at[slot]),
                pltpu.make_async_copy(w_out.at[:, pl.ds(col, BLK)], wo_buf.at[slot], wo_sem.at[slot]))

    def send(slot, target_ref, recv_sem, device):
        return pltpu.make_async_remote_copy(
            src_ref=stage.at[slot], dst_ref=target_ref, send_sem=stage_sem.at[slot], recv_sem=recv_sem,
            device_id=(device,), device_id_type=MESH)

    def to_core(slot, index):
        return send(slot, recv_core.at[index], core_sem.at[index], partner)

    def to_first(slot, index, device):
        return send(slot, recv_first.at[index], first_sem.at[index], device)

    def to_second(slot, index, device):
        return send(slot, recv_second.at[index], second_sem.at[index], device)

    def wait_slot(slot):
        to_core(slot, 0).wait_send()

    shift = 32 * lax.rem(me, 4)

    def moment_loads(sub, half):
        first_row = jnp.clip(BLK * sub - shift, 0, SHARD - BLK)
        place = pl.multiple_of(EDGE + first_row + shift - BLK * sub, 32)
        rows = pl.ds(pl.multiple_of(first_row, 32), BLK)
        return [pltpu.make_async_copy(source.at[rows], moments.at[half, kind, pl.ds(place, BLK)], load_sem.at[half, kind])
                for kind, source in enumerate((mom, var))]

    def edge_loads(half):
        place = pl.ds(pl.multiple_of(BLK + shift, 32), EDGE)
        return [pltpu.make_async_copy(edge.at[kind], moments.at[half, kind, place], edge_sem.at[half, kind])
                for kind in range(2)]

    def moment_stores(sub, half):
        pieces = [(None, EDGE, BLK - 2 * EDGE)]
        for step in range(3):
            pieces.append((jnp.logical_or(sub > 0, 32 * step >= shift), 32 * step, 32))
            pieces.append((jnp.logical_or(sub < SUBS - 1, 32 * step < shift), BLK - EDGE + 32 * step, 32))
        out = []
        for position, (needed, row, size) in enumerate(pieces):
            target = jnp.maximum(BLK * sub - shift + row, 0)
            rows = pl.ds(pl.multiple_of(target, 32), size)
            for kind, result in enumerate((mom_new, var_new)):
                out.append((needed, pltpu.make_async_copy(
                    moments.at[half, kind, pl.ds(EDGE + row, size)], result.at[rows], store_sem.at[half, kind, position])))
        return out

    def weight_stores(sub, half):
        cols = pl.ds(pl.multiple_of(lax.rem(sub, SUBS // 2) * BLK, BLK), BLK)
        return [(sub < SUBS // 2, pltpu.make_async_copy(fin_w.at[half], w_left.at[:, cols], fin_sem.at[half])),
                (sub >= SUBS // 2, pltpu.make_async_copy(fin_w.at[half], w_right.at[:, cols], fin_sem.at[half]))]

    def for_stores(sub, half, action):
        for needed, copy in moment_stores(sub, half) + weight_stores(sub, half):
            if needed is None:
                action(copy)
            else:
                pl.when(needed)(functools.partial(action, copy))

    for copy in fetch(jnp.int32(0)):
        copy.start()
    g_acc[...] = jnp.zeros_like(g_acc)

    def body(n, carry):
        group, half, own, rel, sub, dest, col = decode(n)
        slot = lax.rem(n, 2)

        @pl.when(n + 1 < BLOCKS)
        def _():
            for copy in fetch(n + 1):
                copy.start()

        core_index = sub * 4 + rel
        first_index = sub * 2 + 1 - lax.rem(rel, 2)
        needs_first = jnp.logical_and(own == 1, rel >= 2)
        is_final = jnp.logical_and(own == 1, rel == 3)
        load_core = pltpu.make_async_copy(recv_core.at[core_index], add_core.at[half], add_sem.at[half, 0])
        load_first = pltpu.make_async_copy(recv_first.at[first_index], add_first.at[half], add_sem.at[half, 1])

        for copy in fetch(n):
            copy.wait()

        @pl.loop(0, BLK // 256)
        def _(tile):
            cols = pl.ds(pl.multiple_of(tile * 256, 256), 256)
            acc[half, :, cols] = jnp.dot(hidden_t[...], dz_buf[slot, :, cols], preferred_element_type=jnp.float32)

        @pl.when(own == 1)
        def _():
            to_core(0, core_index).wait_recv()
            load_core.start()

        @pl.when(needs_first)
        def _():
            to_first(0, first_index, near_x).wait_recv()
            load_first.start()

        @pl.when(is_final)
        def _():
            @pl.when(sub >= 2)
            def _():
                for_stores(sub - 2, half, lambda copy: copy.wait())

            for copy in moment_loads(sub, half):
                copy.start()

            @pl.when(sub == SUBS - 1)
            def _():
                for copy in edge_loads(half):
                    copy.start()

            fin_w[half] = wo_buf[slot]

        @pl.when(own == 0)
        def _():
            place = 2 * RING + lax.rem(group, 2) * 2 + half

            @pl.when(group >= 2)
            def _():
                wait_slot(place)

            stage[place] = acc[half]
            to_core(place, core_index).start()

        turn = lookup(group, GROUP_SEND)
        along_y = jnp.where(rel < 2, half, 1 - half)
        place = along_y * RING + lax.rem(turn, RING)
        device = jnp.where(along_y == 1, near_y, near_x)

        @pl.when(jnp.logical_and(own == 1, rel < 2))
        def _():
            load_core.wait()

            @pl.when(turn >= RING)
            def _():
                wait_slot(place)

            stage[place] = acc[half] + add_core[half]
            to_first(place, first_index, device).start()

        @pl.when(jnp.logical_and(own == 1, rel == 2))
        def _():
            load_core.wait()
            load_first.wait()

            @pl.when(turn >= RING)
            def _():
                wait_slot(place)

            stage[place] = acc[half] + add_core[half] + add_first[half]
            to_second(place, sub, device).start()

        lane = lax.broadcasted_iota(jnp.int32, (1, BLK), 1) + (col - SHARD * dest)
        keep = jnp.where(jnp.logical_and(lane >= 0, lane < SHARD), 1.0, 0.0).astype(jnp.bfloat16)
        weights = wo_buf[slot] * keep

        @pl.loop(0, 4)
        def _(tile):
            rows = pl.ds(pl.multiple_of(tile * 512, 512), 512)
            g_acc[rows, :] += lax.dot_general(dz_buf[slot, rows, :], weights, (((1,), (1,)), ((), ())),
                                              preferred_element_type=jnp.float32)

        @pl.when(jnp.logical_and(is_final, half == 1))
        def _():
            for part in range(2):
                this = sub - 1 + part
                to_second(0, this, near_x).wait_recv()
                pltpu.make_async_copy(recv_core.at[this * 4 + 3], add_core.at[part], add_sem.at[part, 0]).wait()
                pltpu.make_async_copy(recv_first.at[this * 2], add_first.at[part], add_sem.at[part, 1]).wait()
                for copy in moment_loads(this, part):
                    copy.wait()

                @pl.when(this == SUBS - 1)
                def _():
                    for copy in edge_loads(part):
                        copy.wait()

            @pl.loop(0, 2 * (BLK // 128))
            def _(tile):
                part = tile // (BLK // 128)
                tile = lax.rem(tile, BLK // 128)
                cols = pl.ds(pl.multiple_of(tile * 128, 128), 128)
                rows = pl.ds(pl.multiple_of(EDGE + tile * 128, 32), 128)
                total = acc[part, :, cols] + add_core[part, :, cols] + add_first[part, :, cols] + recv_second[sub - 1 + part, :, cols]
                first, second, direction = adam_update(total.T, moments[part, 0, rows, :], moments[part, 1, rows, :])
                moments[part, 0, rows, :] = first
                moments[part, 1, rows, :] = second
                fin_w[part, :, cols] = (fin_w[part, :, cols].astype(jnp.float32) - LR_HEAD * direction.T).astype(jnp.bfloat16)

            for part in range(2):
                for_stores(sub - 1 + part, part, lambda copy: copy.start())

        return carry

    lax.fori_loop(0, BLOCKS, body, 0)

    @pl.loop(0, 4)
    def _(tile):
        rows = pl.ds(pl.multiple_of(tile * 512, 512), 512)
        grad_hidden[rows, :] = g_acc[rows, :].astype(jnp.bfloat16)

    for half in range(2):
        for_stores(SUBS - 2 + half, half, lambda copy: copy.wait())
    for place in range(2 * RING + DRING):
        wait_slot(place)


def head_update(hidden, d_logits, w_out, mom_t, var_t, edge):
    tokens, dim = hidden.shape
    f32 = jnp.float32
    bf16 = jnp.bfloat16
    any_spec = pl.BlockSpec(memory_space=pl.ANY)
    vmem = pl.BlockSpec(memory_space=pltpu.VMEM)
    outs = pl.pallas_call(
        head_kernel,
        out_shape=(
            jax.ShapeDtypeStruct((dim, SUBS * BLK // 2), bf16),
            jax.ShapeDtypeStruct((dim, SUBS * BLK // 2), bf16),
            jax.ShapeDtypeStruct(mom_t.shape, f32),
            jax.ShapeDtypeStruct(var_t.shape, f32),
            pltpu.VMEM((tokens, dim), bf16),
            jax.ShapeDtypeStruct((4 * SUBS, dim, BLK), f32),
            jax.ShapeDtypeStruct((2 * SUBS, dim, BLK), f32),
        ),
        in_specs=[vmem] + [any_spec] * 5,
        out_specs=(any_spec, any_spec, any_spec, any_spec, vmem, any_spec, any_spec),
        scratch_shapes=[
            pltpu.VMEM((2, tokens, BLK), bf16),
            pltpu.VMEM((2, dim, BLK), bf16),
            pltpu.VMEM((2, dim, BLK), f32),
            pltpu.VMEM((tokens, dim), f32),
            pltpu.VMEM((2, dim, BLK), f32),
            pltpu.VMEM((2, dim, BLK), f32),
            pltpu.VMEM((SUBS, dim, BLK), f32),
            pltpu.VMEM((2 * RING + DRING, dim, BLK), f32),
            pltpu.VMEM((2, 2, BLK + 2 * EDGE, dim), f32),
            pltpu.VMEM((2, dim, BLK), bf16),
            pltpu.SemaphoreType.DMA((2,)),
            pltpu.SemaphoreType.DMA((2,)),
            pltpu.SemaphoreType.DMA((4 * SUBS,)),
            pltpu.SemaphoreType.DMA((2 * SUBS,)),
            pltpu.SemaphoreType.DMA((SUBS,)),
            pltpu.SemaphoreType.DMA((2 * RING + DRING,)),
            pltpu.SemaphoreType.DMA((2, 2)),
            pltpu.SemaphoreType.DMA((2, 2)),
            pltpu.SemaphoreType.DMA((2, 2)),
            pltpu.SemaphoreType.DMA((2, 2, 7)),
            pltpu.SemaphoreType.DMA((2,)),
        ],
        compiler_params=pltpu.CompilerParams(collective_id=0, has_side_effects=True, vmem_limit_bytes=56 * 1024 * 1024),
        cost_estimate=pl.CostEstimate(flops=280_000_000_000, bytes_accessed=300_000_000, transcendentals=0),
        name='head_update',
    )(hidden.T, d_logits, w_out, mom_t, var_t, edge)
    return outs[:5]


def flip(me, far):
    for bit, weight in zip(far, (2, 4, 1)):
        if bit:
            me = me + weight - 2 * weight * lax.rem(me // weight, 2)
    return me


def permute(value, far):
    mask = 2 * far[0] + 4 * far[1] + far[2]
    return lax.ppermute(value, DATA_AXIS, [(dev, dev ^ mask) for dev in range(8)])


def place_kernel(origins, num_copies, has_base, *refs):
    count = len(origins)
    pieces = refs[:count]
    sources = refs[count:count + num_copies]
    refs = refs[count + num_copies + has_base:]
    out, targets = refs[0], refs[1:1 + num_copies]
    buf, in_sem, out_sem, edge_sem = refs[1 + num_copies:5 + num_copies]
    me = lax.axis_index(DATA_AXIS)
    width = pieces[0].shape[-1]
    loads = [pltpu.make_async_copy(piece, buf.at[position], in_sem.at[position]) for position, piece in enumerate(pieces)]
    for load in loads:
        load.start()
    if num_copies:
        wide, wide_in, wide_out = refs[5 + num_copies:]
        rows = wide.shape[1]
        steps = sources[0].shape[0] // rows
        work = [(kind, step) for step in range(steps) for kind in range(num_copies)]

        def wide_load(index):
            kind, step = work[index]
            return pltpu.make_async_copy(sources[kind].at[pl.ds(step * rows, rows)], wide.at[index % 4], wide_in.at[index % 4])

        def wide_store(index):
            kind, step = work[index]
            return pltpu.make_async_copy(wide.at[index % 4], targets[kind].at[pl.ds(step * rows, rows)], wide_out.at[index % 4])

        for index in range(2):
            wide_load(index).start()
        for index in range(len(work)):
            wide_load(index).wait()
            wide_store(index).start()
            if index + 2 < len(work):
                if index >= 2:
                    wide_store(index - 2).wait()
                wide_load(index + 2).start()
        for index in range(len(work) - 4, len(work)):
            wide_store(index).wait()
    stores = []
    for position, (far, part) in enumerate(origins):
        loads[position].wait()
        dest = flip(me, far)
        col = pl.multiple_of(((125 * dest) // 4) * 128 + part * width, 128)
        skip = 0 if part else 128
        store = pltpu.make_async_copy(buf.at[position, :, pl.ds(skip, width - skip)],
                                      out.at[:, pl.ds(pl.multiple_of(col + skip, 128), width - skip)], out_sem.at[position])
        store.start()
        stores.append(store)
        if not part:
            edge = pltpu.make_async_copy(buf.at[position, :, pl.ds(0, 128)], out.at[:, pl.ds(col, 128)], edge_sem.at[position])

            @pl.when(lax.rem(dest, 4) == 0)
            def _():
                edge.start()
                edge.wait()
    for store in stores:
        store.wait()


def place(base, placed, vocab, copies=()):
    pieces = [piece for piece, _, _ in placed]
    origins = tuple((far, part) for _, far, part in placed)
    dim, width = pieces[0].shape
    count = len(pieces)
    has_base = base is not None
    args = pieces + list(copies) + ([base] if has_base else [])
    scratch = [pltpu.VMEM((count, dim, width), jnp.bfloat16)] + [pltpu.SemaphoreType.DMA((count,))] * 3
    if copies:
        scratch += [pltpu.VMEM((4, 400, dim), jnp.float32), pltpu.SemaphoreType.DMA((4,)), pltpu.SemaphoreType.DMA((4,))]
    any_spec = pl.BlockSpec(memory_space=pl.ANY)
    outs = pl.pallas_call(
        functools.partial(place_kernel, origins, len(copies), int(has_base)),
        out_shape=[jax.ShapeDtypeStruct((dim, vocab), jnp.bfloat16)] + [jax.ShapeDtypeStruct(c.shape, c.dtype) for c in copies],
        in_specs=[any_spec] * len(args),
        out_specs=[any_spec] * (1 + len(copies)),
        scratch_shapes=scratch,
        input_output_aliases={len(args) - 1: 0} if has_base else {},
        compiler_params=pltpu.CompilerParams(vmem_limit_bytes=40 * 1024 * 1024),
        cost_estimate=pl.CostEstimate(flops=6_000_000_000 if copies else 3_000_000_000, bytes_accessed=count * 4 * dim * width, transcendentals=0),
        name='place',
    )(*args)
    return outs


NEAR = ((1, 0), (0, 1), (1, 1))


def small_kernel(up_0, up_1, down_0, down_1, mom, var, mom_new, var_new, dir_up, dir_down,
                 parts, dirs, whole, from_core, from_chip, stage,
                 core_send, core_recv, chip_send, chip_recv, gather_send, gather_recv, back_send, back_recv):
    me = lax.axis_index(DATA_AXIS)
    partner = flip(me, (0, 0, 1))
    chips = [me] + [flip(me, far + (0,)) for far in NEAR]
    barrier = pltpu.get_barrier_semaphore()
    for other in chips[1:] + [partner]:
        pl.semaphore_signal(barrier, inc=1, device_id=(other,), device_id_type=MESH)
    pl.semaphore_wait(barrier, 4)

    shard = parts.shape[2]
    lows = (up_0, up_1, down_0, down_1)
    for dev in range(parts.shape[0]):
        for kind, low in enumerate(lows):
            parts[dev, kind] = low[dev * shard:(dev + 1) * shard, :]

    def remote(source, target, send_sem, recv_sem, device):
        return pltpu.make_async_remote_copy(src_ref=source, dst_ref=target, send_sem=send_sem, recv_sem=recv_sem,
                                            device_id=(device,), device_id_type=MESH)

    order = (1, 2, 3, 0)
    to_core = {}
    for k in order:
        to_core[k] = remote(parts.at[flip(chips[k], (0, 0, 1))], from_core.at[k], core_send.at[k], core_recv.at[k], partner)
        to_core[k].start()
    to_chip = []
    for k in (1, 2, 3):
        to_core[k].wait_recv()
        stage[k - 1] = parts[chips[k]] + from_core[k]
        copy = remote(stage.at[k - 1], from_chip.at[k - 1], chip_send.at[k - 1], chip_recv.at[k - 1], chips[k])
        copy.start()
        to_chip.append(copy)
    to_core[0].wait_recv()
    for copy in to_chip:
        copy.wait_recv()
    total = parts[me] + from_core[0] + from_chip[0] + from_chip[1] + from_chip[2]
    first, second, direction = adam_update(total, mom[...], var[...])
    mom_new[...] = first
    var_new[...] = second
    dirs[me] = direction.astype(jnp.bfloat16)
    gather = [remote(dirs.at[me], dirs.at[me], gather_send.at[k - 1], gather_recv.at[k - 1], chips[k]) for k in (1, 2, 3)]
    back = [remote(dirs.at[chips[k]], dirs.at[chips[k]], back_send.at[k], back_recv.at[k], partner) for k in range(4)]
    for copy in gather:
        copy.start()
    back[0].start()
    for k in (1, 2, 3):
        remote(dirs.at[chips[k]], dirs.at[chips[k]], gather_send.at[k - 1], gather_recv.at[k - 1], chips[k]).wait_recv()
        back[k].start()
    for k in range(4):
        remote(dirs.at[flip(chips[k], (0, 0, 1))], dirs.at[flip(chips[k], (0, 0, 1))], back_send.at[k], back_recv.at[k], partner).wait_recv()
        back[k].wait_send()
        to_core[k].wait_send()
    for copy in gather + to_chip:
        copy.wait_send()
    for kind in range(4):
        for dev in range(parts.shape[0]):
            whole[dev * shard:(dev + 1) * shard, :] = dirs[dev, kind].astype(jnp.float32)
        target = dir_up if kind < 2 else dir_down
        target[kind % 2] = whole[...].astype(jnp.bfloat16)


def small_update(lows, mom, var):
    shape = mom.shape
    rows, rank = lows[0].shape
    devices = rows // shape[1]
    f32 = jnp.float32
    vmem = pl.BlockSpec(memory_space=pltpu.VMEM)
    dma = pltpu.SemaphoreType.DMA
    return pl.pallas_call(
        small_kernel,
        out_shape=(jax.ShapeDtypeStruct(shape, f32), jax.ShapeDtypeStruct(shape, f32),
                   jax.ShapeDtypeStruct((2, rows, rank), jnp.bfloat16), jax.ShapeDtypeStruct((2, rows, rank), jnp.bfloat16)),
        in_specs=[vmem] * 6,
        out_specs=(vmem,) * 4,
        scratch_shapes=[pltpu.VMEM((devices,) + shape, f32), pltpu.VMEM((devices,) + shape, jnp.bfloat16),
                        pltpu.VMEM((rows, rank), f32), pltpu.VMEM((4,) + shape, f32), pltpu.VMEM((3,) + shape, f32), pltpu.VMEM((3,) + shape, f32),
                        dma((4,)), dma((4,)), dma((3,)), dma((3,)), dma((3,)), dma((3,)), dma((4,)), dma((4,))],
        compiler_params=pltpu.CompilerParams(collective_id=1, has_side_effects=True, vmem_limit_bytes=32 * 1024 * 1024),
        cost_estimate=pl.CostEstimate(flops=30_000_000_000, bytes_accessed=10_000_000, transcendentals=0),
        name='small_update',
    )(*lows, mom, var)


def local_step(tokens, d_logits, w_up, w_down, w_out, proj_up, proj_down, mom_up, var_up, mom_down, var_down, mom_out, var_out):
    num_layers = w_up.shape[0]
    hidden = tokens
    saved_acts = []
    for layer_idx in range(num_layers):
        pre_act = jnp.dot(hidden, w_up[layer_idx], preferred_element_type=jnp.float32).astype(jnp.bfloat16)
        post_act = gelu_tanh(pre_act.astype(jnp.float32)).astype(jnp.bfloat16)
        saved_acts.append((hidden, pre_act, post_act))
        hidden = (hidden.astype(jnp.float32) + jnp.dot(post_act, w_down[layer_idx], preferred_element_type=jnp.float32)).astype(jnp.bfloat16)

    devices = lax.axis_size(DATA_AXIS)
    mom_t, var_t = mom_out.T, var_out.T
    edge = lax.ppermute(jnp.stack([mom_t[:EDGE], var_t[:EDGE]]), DATA_AXIS, [(dev, dev - 1) for dev in range(1, devices)])
    left, right, m_raw, v_raw, grad_hidden = head_update(hidden, d_logits, w_out, mom_t, var_t, edge)
    far_x, far_y, far_xy, near = (1, 0, 0), (0, 1, 0), (1, 1, 0), (0, 0, 0)
    left_x = permute(left, far_x)
    right_y = permute(right, far_y)

    def with_core(pieces):
        return pieces + [(permute(piece, (0, 0, 1)), (far[0], far[1], 1), part) for piece, far, part in pieces]

    ups = []
    downs = []
    for layer_idx in reversed(range(num_layers)):
        hidden_in, pre_act, post_act = saved_acts[layer_idx]
        grad_down = jnp.einsum('tf,td->fd', post_act, grad_hidden, preferred_element_type=jnp.float32)
        d_post = jnp.einsum('td,fd->tf', grad_hidden, w_down[layer_idx], preferred_element_type=jnp.float32)
        gelu_pull = jax.vjp(gelu_tanh, pre_act.astype(jnp.float32))[1]
        d_pre = gelu_pull(d_post)[0].astype(jnp.bfloat16)
        if layer_idx == num_layers - 1:
            d_pre, left, right = lax.optimization_barrier((d_pre, left, right))
            left_y = permute(left, far_y)
            right_x = permute(right, far_x)
        else:
            d_pre = lax.optimization_barrier(d_pre)
        grad_up = jnp.einsum('tf,td->fd', d_pre, hidden_in, preferred_element_type=jnp.float32)
        if layer_idx > 0:
            grad_hidden = (grad_hidden.astype(jnp.float32) + jnp.einsum('tf,df->td', d_pre, w_up[layer_idx], preferred_element_type=jnp.float32)).astype(jnp.bfloat16)
        low_up = jnp.dot(grad_up, proj_up[layer_idx].astype(jnp.float32), preferred_element_type=jnp.float32)
        low_down = jnp.dot(grad_down, proj_down[layer_idx].astype(jnp.float32), preferred_element_type=jnp.float32)
        ups.append(low_up)
        downs.append(low_down)
    ups = ups[::-1]
    downs = downs[::-1]

    vocab = d_logits.shape[1]
    ups[0], downs[0], left_x, right_y = lax.optimization_barrier((ups[0], downs[0], left_x, right_y))
    left_xy = permute(left_x, far_y)
    right_xy = permute(right_y, far_x)
    own_pieces = with_core([(left, near, 0), (right, near, 1)])
    w_new, m_out, v_out = place(None, own_pieces, vocab, (m_raw, v_raw))
    w_new, = place(w_new, with_core([(left_x, far_x, 0), (right_y, far_y, 1)]), vocab)

    w_new, left_y, right_x = lax.optimization_barrier((w_new, left_y, right_x))
    w_new, = place(w_new, with_core([(left_y, far_y, 0), (right_x, far_x, 1)]), vocab)
    first = jnp.concatenate([jnp.swapaxes(mom_up, 1, 2), mom_down], axis=0)
    second = jnp.concatenate([jnp.swapaxes(var_up, 1, 2), var_down], axis=0)
    lows = ups + downs
    w_new, lows[0] = lax.optimization_barrier((w_new, lows[0]))
    m_low, v_low, dir_up, dir_down = small_update(lows, first, second)
    m_low, left_xy, right_xy = lax.optimization_barrier((m_low, left_xy, right_xy))
    step_up = jnp.einsum('ldr,lfr->ldf', proj_up, dir_up, preferred_element_type=jnp.float32)
    step_down = jnp.einsum('lfr,ldr->lfd', dir_down, proj_down, preferred_element_type=jnp.float32)
    w_up_new = (w_up.astype(jnp.float32) - LR * ALPHA * step_up).astype(jnp.bfloat16)
    w_down_new = (w_down.astype(jnp.float32) - LR * ALPHA * step_down).astype(jnp.bfloat16)

    w_out_new, = place(w_new, with_core([(left_xy, far_xy, 0), (right_xy, far_xy, 1)]), vocab)

    return (w_up_new, w_down_new, w_out_new,
            jnp.swapaxes(m_low[:num_layers], 1, 2), jnp.swapaxes(v_low[:num_layers], 1, 2),
            m_low[num_layers:], v_low[num_layers:],
            m_out.T, v_out.T)


def solution(mesh):
    row_spec = P(DATA_AXIS, None)
    whole = P()
    up_spec = P(None, None, DATA_AXIS)
    down_spec = P(None, DATA_AXIS, None)
    head_spec = P(None, DATA_AXIS)
    in_specs = (row_spec, row_spec, whole, whole, whole, whole, whole, up_spec, up_spec, down_spec, down_spec, head_spec, head_spec)
    out_specs = (whole, whole, whole, up_spec, up_spec, down_spec, down_spec, head_spec, head_spec)
    return jax.shard_map(local_step, mesh=mesh, in_specs=in_specs, out_specs=out_specs, check_vma=False)
```

```python
import functools

import jax
import jax.numpy as jnp
from jax import lax
from jax.experimental import pallas as pl
from jax.experimental.pallas import tpu as pltpu
from jax.sharding import PartitionSpec as P


BETA1 = 0.9
BETA2 = 0.999
EPS = 1e-8
STEP = 4
LR = 0.02
ALPHA = 0.5
LR_HEAD = 0.01
DATA_AXIS = 'data'
MESH = pl.DeviceIdType.MESH

BLK = 512
SUBS = 8
SHARD = 4000
RING = 6
EDGE = 96
DRING = 4

GROUP_DEST = (0, 1, 0, 1, 2, 0, 1, 2, 3, 0, 1, 2, 3, 2, 3, 3)
GROUP_PAIR = (0, 0, 1, 1, 0, 2, 2, 1, 0, 3, 3, 2, 1, 3, 2, 3)
GROUP_SEND = (0, 1, 2, 3, 4, 5, 6, 7, 0, 8, 9, 10, 0, 11, 0, 0)
BLOCKS = 64


def lookup(index, values):
    out = jnp.int32(values[-1])
    for position in range(len(values) - 1):
        out = jnp.where(index == position, jnp.int32(values[position]), out)
    return out


def gelu_tanh(values):
    return jax.nn.gelu(values, approximate=True)


def adam_update(gradient, moment_one, moment_two):
    moment_one = BETA1 * moment_one + (1.0 - BETA1) * gradient
    moment_two = BETA2 * moment_two + (1.0 - BETA2) * gradient * gradient
    direction = (moment_one / (1.0 - BETA1 ** STEP)) / (jnp.sqrt(moment_two / (1.0 - BETA2 ** STEP)) + EPS)
    return moment_one, moment_two, direction


def head_kernel(hidden, d_logits, w_out, mom, var, edge,
                w_left, w_right, mom_new, var_new, grad_hidden, recv_core, recv_first,
                hidden_t, dz_buf, wo_buf, acc, g_acc, add_core, add_first, recv_second, stage, moments, fin_w,
                dz_sem, wo_sem, core_sem, first_sem, second_sem, stage_sem, add_sem, load_sem, edge_sem, store_sem, fin_sem):
    me = lax.axis_index(DATA_AXIS)
    core = lax.rem(me, 2)
    pos_x = lax.rem(me // 2, 2)
    pos_y = me // 4
    partner = me + 1 - 2 * core
    near_x = me + 2 - 4 * pos_x
    near_y = me + 4 - 8 * pos_y

    def decode(n):
        group = n // 4
        half = lax.rem(n, 2)
        own = lax.rem(n // 2, 2)
        rel = lookup(group, GROUP_DEST)
        far_first = 1 - rel // 2
        far_second = 1 - lax.rem(rel, 2)
        sub = 2 * lookup(group, GROUP_PAIR) + half
        delta_x = jnp.where(half == 0, far_first, far_second)
        delta_y = jnp.where(half == 0, far_second, far_first)
        dest_x = pos_x + delta_x - 2 * pos_x * delta_x
        dest_y = pos_y + delta_y - 2 * pos_y * delta_y
        dest_core = jnp.where(own == 1, core, 1 - core)
        dest = (dest_y * 2 + dest_x) * 2 + dest_core
        col = pl.multiple_of(((125 * dest) // 4 + 4 * sub) * 128, 128)
        return group, half, own, rel, sub, dest, col

    def fetch(n):
        col = decode(n)[-1]
        slot = lax.rem(n, 2)
        return (pltpu.make_async_copy(d_logits.at[:, pl.ds(col, BLK)], dz_buf.at[slot], dz_sem.at[slot]),
                pltpu.make_async_copy(w_out.at[:, pl.ds(col, BLK)], wo_buf.at[slot], wo_sem.at[slot]))

    def send(slot, target_ref, recv_sem, device):
        return pltpu.make_async_remote_copy(
            src_ref=stage.at[slot], dst_ref=target_ref, send_sem=stage_sem.at[slot], recv_sem=recv_sem,
            device_id=(device,), device_id_type=MESH)

    def to_core(slot, index):
        return send(slot, recv_core.at[index], core_sem.at[index], partner)

    def to_first(slot, index, device):
        return send(slot, recv_first.at[index], first_sem.at[index], device)

    def to_second(slot, index, device):
        return send(slot, recv_second.at[index], second_sem.at[index], device)

    def wait_slot(slot):
        to_core(slot, 0).wait_send()

    shift = 32 * lax.rem(me, 4)

    def moment_loads(sub, half):
        first_row = jnp.clip(BLK * sub - shift, 0, SHARD - BLK)
        place = pl.multiple_of(EDGE + first_row + shift - BLK * sub, 32)
        rows = pl.ds(pl.multiple_of(first_row, 32), BLK)
        return [pltpu.make_async_copy(source.at[rows], moments.at[half, kind, pl.ds(place, BLK)], load_sem.at[half, kind])
                for kind, source in enumerate((mom, var))]

    def edge_loads(half):
        place = pl.ds(pl.multiple_of(BLK + shift, 32), EDGE)
        return [pltpu.make_async_copy(edge.at[kind], moments.at[half, kind, place], edge_sem.at[half, kind])
                for kind in range(2)]

    def moment_stores(sub, half):
        pieces = [(None, EDGE, BLK - 2 * EDGE)]
        for step in range(3):
            pieces.append((jnp.logical_or(sub > 0, 32 * step >= shift), 32 * step, 32))
            pieces.append((jnp.logical_or(sub < SUBS - 1, 32 * step < shift), BLK - EDGE + 32 * step, 32))
        out = []
        for position, (needed, row, size) in enumerate(pieces):
            target = jnp.maximum(BLK * sub - shift + row, 0)
            rows = pl.ds(pl.multiple_of(target, 32), size)
            for kind, result in enumerate((mom_new, var_new)):
                out.append((needed, pltpu.make_async_copy(
                    moments.at[half, kind, pl.ds(EDGE + row, size)], result.at[rows], store_sem.at[half, kind, position])))
        return out

    def weight_stores(sub, half):
        cols = pl.ds(pl.multiple_of(lax.rem(sub, SUBS // 2) * BLK, BLK), BLK)
        return [(sub < SUBS // 2, pltpu.make_async_copy(fin_w.at[half], w_left.at[:, cols], fin_sem.at[half])),
                (sub >= SUBS // 2, pltpu.make_async_copy(fin_w.at[half], w_right.at[:, cols], fin_sem.at[half]))]

    def for_stores(sub, half, action):
        for needed, copy in moment_stores(sub, half) + weight_stores(sub, half):
            if needed is None:
                action(copy)
            else:
                pl.when(needed)(functools.partial(action, copy))

    for copy in fetch(jnp.int32(0)):
        copy.start()
    barrier = pltpu.get_barrier_semaphore()
    for other in (partner, near_x, near_y):
        pl.semaphore_signal(barrier, inc=1, device_id=(other,), device_id_type=MESH)

    @pl.loop(0, hidden.shape[0] // 512)
    def _(tile):
        rows = pl.ds(pl.multiple_of(tile * 512, 512), 512)
        hidden_t[:, rows] = hidden[rows, :].T

    g_acc[...] = jnp.zeros_like(g_acc)
    pl.semaphore_wait(barrier, 3)


    def body(n, carry):
        group, half, own, rel, sub, dest, col = decode(n)
        slot = lax.rem(n, 2)

        @pl.when(n + 1 < BLOCKS)
        def _():
            for copy in fetch(n + 1):
                copy.start()

        core_index = sub * 4 + rel
        first_index = sub * 2 + 1 - lax.rem(rel, 2)
        needs_first = jnp.logical_and(own == 1, rel >= 2)
        is_final = jnp.logical_and(own == 1, rel == 3)
        load_core = pltpu.make_async_copy(recv_core.at[core_index], add_core.at[half], add_sem.at[half, 0])
        load_first = pltpu.make_async_copy(recv_first.at[first_index], add_first.at[half], add_sem.at[half, 1])

        @pl.when(own == 1)
        def _():
            to_core(0, core_index).wait_recv()
            load_core.start()

        @pl.when(needs_first)
        def _():
            to_first(0, first_index, near_x).wait_recv()
            load_first.start()

        for copy in fetch(n):
            copy.wait()

        @pl.loop(0, BLK // 256)
        def _(tile):
            cols = pl.ds(pl.multiple_of(tile * 256, 256), 256)
            acc[half, :, cols] = jnp.dot(hidden_t[...], dz_buf[slot, :, cols], preferred_element_type=jnp.float32)

        @pl.when(is_final)
        def _():
            @pl.when(sub >= 2)
            def _():
                for_stores(sub - 2, half, lambda copy: copy.wait())

            for copy in moment_loads(sub, half):
                copy.start()

            @pl.when(sub == SUBS - 1)
            def _():
                for copy in edge_loads(half):
                    copy.start()

            fin_w[half] = wo_buf[slot]

        @pl.when(own == 0)
        def _():
            place = 2 * RING + lax.rem(group, 2) * 2 + half

            @pl.when(group >= 2)
            def _():
                wait_slot(place)

            stage[place] = acc[half]
            to_core(place, core_index).start()

        turn = lookup(group, GROUP_SEND)
        along_y = jnp.where(rel < 2, half, 1 - half)
        place = along_y * RING + lax.rem(turn, RING)
        device = jnp.where(along_y == 1, near_y, near_x)

        @pl.when(jnp.logical_and(own == 1, rel < 2))
        def _():
            load_core.wait()

            @pl.when(turn >= RING)
            def _():
                wait_slot(place)

            stage[place] = acc[half] + add_core[half]
            to_first(place, first_index, device).start()

        @pl.when(jnp.logical_and(own == 1, rel == 2))
        def _():
            load_core.wait()
            load_first.wait()

            @pl.when(turn >= RING)
            def _():
                wait_slot(place)

            stage[place] = acc[half] + add_core[half] + add_first[half]
            to_second(place, sub, device).start()

        lane = lax.broadcasted_iota(jnp.int32, (1, BLK), 1) + (col - SHARD * dest)
        keep = jnp.where(jnp.logical_and(lane >= 0, lane < SHARD), 1.0, 0.0).astype(jnp.bfloat16)
        weights = wo_buf[slot] * keep

        @pl.loop(0, 4)
        def _(tile):
            rows = pl.ds(pl.multiple_of(tile * 512, 512), 512)
            g_acc[rows, :] += lax.dot_general(dz_buf[slot, rows, :], weights, (((1,), (1,)), ((), ())),
                                              preferred_element_type=jnp.float32)

        @pl.when(jnp.logical_and(is_final, half == 1))
        def _():
            for part in range(2):
                this = sub - 1 + part
                to_second(0, this, near_x).wait_recv()
                pltpu.make_async_copy(recv_core.at[this * 4 + 3], add_core.at[part], add_sem.at[part, 0]).wait()
                pltpu.make_async_copy(recv_first.at[this * 2], add_first.at[part], add_sem.at[part, 1]).wait()
                for copy in moment_loads(this, part):
                    copy.wait()

                @pl.when(this == SUBS - 1)
                def _():
                    for copy in edge_loads(part):
                        copy.wait()

            @pl.loop(0, 2 * (BLK // 128))
            def _(tile):
                part = tile // (BLK // 128)
                tile = lax.rem(tile, BLK // 128)
                cols = pl.ds(pl.multiple_of(tile * 128, 128), 128)
                rows = pl.ds(pl.multiple_of(EDGE + tile * 128, 32), 128)
                total = acc[part, :, cols] + add_core[part, :, cols] + add_first[part, :, cols] + recv_second[sub - 1 + part, :, cols]
                first, second, direction = adam_update(total.T, moments[part, 0, rows, :], moments[part, 1, rows, :])
                moments[part, 0, rows, :] = first
                moments[part, 1, rows, :] = second
                fin_w[part, :, cols] = (fin_w[part, :, cols].astype(jnp.float32) - LR_HEAD * direction.T).astype(jnp.bfloat16)

            for part in range(2):
                for_stores(sub - 1 + part, part, lambda copy: copy.start())

        return carry

    lax.fori_loop(0, BLOCKS, body, 0)

    @pl.loop(0, 4)
    def _(tile):
        rows = pl.ds(pl.multiple_of(tile * 512, 512), 512)
        grad_hidden[rows, :] = g_acc[rows, :].astype(jnp.bfloat16)

    for half in range(2):
        for_stores(SUBS - 2 + half, half, lambda copy: copy.wait())
    for place in range(2 * RING + DRING):
        wait_slot(place)


def head_update(hidden, d_logits, w_out, mom_t, var_t, edge):
    tokens, dim = hidden.shape
    f32 = jnp.float32
    bf16 = jnp.bfloat16
    any_spec = pl.BlockSpec(memory_space=pl.ANY)
    vmem = pl.BlockSpec(memory_space=pltpu.VMEM)
    outs = pl.pallas_call(
        head_kernel,
        out_shape=(
            jax.ShapeDtypeStruct((dim, SUBS * BLK // 2), bf16),
            jax.ShapeDtypeStruct((dim, SUBS * BLK // 2), bf16),
            jax.ShapeDtypeStruct(mom_t.shape, f32),
            jax.ShapeDtypeStruct(var_t.shape, f32),
            pltpu.VMEM((tokens, dim), bf16),
            jax.ShapeDtypeStruct((4 * SUBS, dim, BLK), f32),
            jax.ShapeDtypeStruct((2 * SUBS, dim, BLK), f32),
        ),
        in_specs=[vmem] + [any_spec] * 5,
        out_specs=(any_spec, any_spec, any_spec, any_spec, vmem, any_spec, any_spec),
        scratch_shapes=[
            pltpu.VMEM((dim, tokens), bf16),
            pltpu.VMEM((2, tokens, BLK), bf16),
            pltpu.VMEM((2, dim, BLK), bf16),
            pltpu.VMEM((2, dim, BLK), f32),
            pltpu.VMEM((tokens, dim), f32),
            pltpu.VMEM((2, dim, BLK), f32),
            pltpu.VMEM((2, dim, BLK), f32),
            pltpu.VMEM((SUBS, dim, BLK), f32),
            pltpu.VMEM((2 * RING + DRING, dim, BLK), f32),
            pltpu.VMEM((2, 2, BLK + 2 * EDGE, dim), f32),
            pltpu.VMEM((2, dim, BLK), bf16),
            pltpu.SemaphoreType.DMA((2,)),
            pltpu.SemaphoreType.DMA((2,)),
            pltpu.SemaphoreType.DMA((4 * SUBS,)),
            pltpu.SemaphoreType.DMA((2 * SUBS,)),
            pltpu.SemaphoreType.DMA((SUBS,)),
            pltpu.SemaphoreType.DMA((2 * RING + DRING,)),
            pltpu.SemaphoreType.DMA((2, 2)),
            pltpu.SemaphoreType.DMA((2, 2)),
            pltpu.SemaphoreType.DMA((2, 2)),
            pltpu.SemaphoreType.DMA((2, 2, 7)),
            pltpu.SemaphoreType.DMA((2,)),
        ],
        compiler_params=pltpu.CompilerParams(collective_id=0, has_side_effects=True, vmem_limit_bytes=56 * 1024 * 1024),
        cost_estimate=pl.CostEstimate(flops=280_000_000_000, bytes_accessed=300_000_000, transcendentals=0),
        name='head_update',
    )(hidden, d_logits, w_out, mom_t, var_t, edge)
    return outs[:5]


def flip(me, far):
    for bit, weight in zip(far, (2, 4, 1)):
        if bit:
            me = me + weight - 2 * weight * lax.rem(me // weight, 2)
    return me


def permute(value, far):
    mask = 2 * far[0] + 4 * far[1] + far[2]
    return lax.ppermute(value, DATA_AXIS, [(dev, dev ^ mask) for dev in range(8)])


def place_kernel(origins, num_copies, has_base, *refs):
    count = len(origins)
    pieces = refs[:count]
    sources = refs[count:count + num_copies]
    refs = refs[count + num_copies + has_base:]
    out, targets = refs[0], refs[1:1 + num_copies]
    buf, in_sem, out_sem, edge_sem = refs[1 + num_copies:5 + num_copies]
    me = lax.axis_index(DATA_AXIS)
    width = pieces[0].shape[-1]
    loads = [pltpu.make_async_copy(piece, buf.at[position], in_sem.at[position]) for position, piece in enumerate(pieces)]
    for load in loads:
        load.start()
    if num_copies:
        wide, wide_in, wide_out = refs[5 + num_copies:]
        rows = wide.shape[1]
        steps = sources[0].shape[0] // rows
        work = [(kind, step) for step in range(steps) for kind in range(num_copies)]

        def wide_load(index):
            kind, step = work[index]
            return pltpu.make_async_copy(sources[kind].at[pl.ds(step * rows, rows)], wide.at[index % 4], wide_in.at[index % 4])

        def wide_store(index):
            kind, step = work[index]
            return pltpu.make_async_copy(wide.at[index % 4], targets[kind].at[pl.ds(step * rows, rows)], wide_out.at[index % 4])

        for index in range(2):
            wide_load(index).start()
        for index in range(len(work)):
            wide_load(index).wait()
            wide_store(index).start()
            if index + 2 < len(work):
                if index >= 2:
                    wide_store(index - 2).wait()
                wide_load(index + 2).start()
        for index in range(len(work) - 4, len(work)):
            wide_store(index).wait()
    stores = []
    for position, (far, part) in enumerate(origins):
        loads[position].wait()
        dest = flip(me, far)
        col = pl.multiple_of(((125 * dest) // 4) * 128 + part * width, 128)
        skip = 0 if part else 128
        store = pltpu.make_async_copy(buf.at[position, :, pl.ds(skip, width - skip)],
                                      out.at[:, pl.ds(pl.multiple_of(col + skip, 128), width - skip)], out_sem.at[position])
        store.start()
        stores.append(store)
        if not part:
            edge = pltpu.make_async_copy(buf.at[position, :, pl.ds(0, 128)], out.at[:, pl.ds(col, 128)], edge_sem.at[position])

            @pl.when(lax.rem(dest, 4) == 0)
            def _():
                edge.start()
                edge.wait()
    for store in stores:
        store.wait()


def place(base, placed, vocab, copies=()):
    pieces = [piece for piece, _, _ in placed]
    origins = tuple((far, part) for _, far, part in placed)
    dim, width = pieces[0].shape
    count = len(pieces)
    has_base = base is not None
    args = pieces + list(copies) + ([base] if has_base else [])
    scratch = [pltpu.VMEM((count, dim, width), jnp.bfloat16)] + [pltpu.SemaphoreType.DMA((count,))] * 3
    if copies:
        scratch += [pltpu.VMEM((4, 400, dim), jnp.float32), pltpu.SemaphoreType.DMA((4,)), pltpu.SemaphoreType.DMA((4,))]
    any_spec = pl.BlockSpec(memory_space=pl.ANY)
    outs = pl.pallas_call(
        functools.partial(place_kernel, origins, len(copies), int(has_base)),
        out_shape=[jax.ShapeDtypeStruct((dim, vocab), jnp.bfloat16)] + [jax.ShapeDtypeStruct(c.shape, c.dtype) for c in copies],
        in_specs=[any_spec] * len(args),
        out_specs=[any_spec] * (1 + len(copies)),
        scratch_shapes=scratch,
        input_output_aliases={len(args) - 1: 0} if has_base else {},
        compiler_params=pltpu.CompilerParams(vmem_limit_bytes=40 * 1024 * 1024),
        cost_estimate=pl.CostEstimate(flops=6_000_000_000 if copies else 3_000_000_000, bytes_accessed=count * 4 * dim * width, transcendentals=0),
        name='place',
    )(*args)
    return outs


NEAR = ((1, 0), (0, 1), (1, 1))


def small_kernel(up_0, up_1, down_0, down_1, mom, var, mom_new, var_new, dir_up, dir_down,
                 parts, dirs, whole, from_core, from_chip, stage,
                 core_send, core_recv, chip_send, chip_recv, gather_send, gather_recv, back_send, back_recv):
    me = lax.axis_index(DATA_AXIS)
    partner = flip(me, (0, 0, 1))
    chips = [me] + [flip(me, far + (0,)) for far in NEAR]
    barrier = pltpu.get_barrier_semaphore()
    for other in chips[1:] + [partner]:
        pl.semaphore_signal(barrier, inc=1, device_id=(other,), device_id_type=MESH)
    pl.semaphore_wait(barrier, 4)

    shard = parts.shape[2]
    lows = (up_0, up_1, down_0, down_1)
    for dev in range(parts.shape[0]):
        for kind, low in enumerate(lows):
            parts[dev, kind] = low[dev * shard:(dev + 1) * shard, :]

    def remote(source, target, send_sem, recv_sem, device):
        return pltpu.make_async_remote_copy(src_ref=source, dst_ref=target, send_sem=send_sem, recv_sem=recv_sem,
                                            device_id=(device,), device_id_type=MESH)

    order = (1, 2, 3, 0)
    to_core = {}
    for k in order:
        to_core[k] = remote(parts.at[flip(chips[k], (0, 0, 1))], from_core.at[k], core_send.at[k], core_recv.at[k], partner)
        to_core[k].start()
    to_chip = []
    for k in (1, 2, 3):
        to_core[k].wait_recv()
        stage[k - 1] = parts[chips[k]] + from_core[k]
        copy = remote(stage.at[k - 1], from_chip.at[k - 1], chip_send.at[k - 1], chip_recv.at[k - 1], chips[k])
        copy.start()
        to_chip.append(copy)
    to_core[0].wait_recv()
    for copy in to_chip:
        copy.wait_recv()
    total = parts[me] + from_core[0] + from_chip[0] + from_chip[1] + from_chip[2]
    first, second, direction = adam_update(total, mom[...], var[...])
    mom_new[...] = first
    var_new[...] = second
    dirs[me] = direction.astype(jnp.bfloat16)
    gather = [remote(dirs.at[me], dirs.at[me], gather_send.at[k - 1], gather_recv.at[k - 1], chips[k]) for k in (1, 2, 3)]
    back = [remote(dirs.at[chips[k]], dirs.at[chips[k]], back_send.at[k], back_recv.at[k], partner) for k in range(4)]
    for copy in gather:
        copy.start()
    back[0].start()
    for k in (1, 2, 3):
        remote(dirs.at[chips[k]], dirs.at[chips[k]], gather_send.at[k - 1], gather_recv.at[k - 1], chips[k]).wait_recv()
        back[k].start()
    for k in range(4):
        remote(dirs.at[flip(chips[k], (0, 0, 1))], dirs.at[flip(chips[k], (0, 0, 1))], back_send.at[k], back_recv.at[k], partner).wait_recv()
        back[k].wait_send()
        to_core[k].wait_send()
    for copy in gather + to_chip:
        copy.wait_send()
    for kind in range(4):
        for dev in range(parts.shape[0]):
            whole[dev * shard:(dev + 1) * shard, :] = dirs[dev, kind].astype(jnp.float32)
        target = dir_up if kind < 2 else dir_down
        target[kind % 2] = whole[...].astype(jnp.bfloat16)


def small_update(lows, mom, var):
    shape = mom.shape
    rows, rank = lows[0].shape
    devices = rows // shape[1]
    f32 = jnp.float32
    vmem = pl.BlockSpec(memory_space=pltpu.VMEM)
    dma = pltpu.SemaphoreType.DMA
    return pl.pallas_call(
        small_kernel,
        out_shape=(jax.ShapeDtypeStruct(shape, f32), jax.ShapeDtypeStruct(shape, f32),
                   jax.ShapeDtypeStruct((2, rows, rank), jnp.bfloat16), jax.ShapeDtypeStruct((2, rows, rank), jnp.bfloat16)),
        in_specs=[vmem] * 6,
        out_specs=(vmem,) * 4,
        scratch_shapes=[pltpu.VMEM((devices,) + shape, f32), pltpu.VMEM((devices,) + shape, jnp.bfloat16),
                        pltpu.VMEM((rows, rank), f32), pltpu.VMEM((4,) + shape, f32), pltpu.VMEM((3,) + shape, f32), pltpu.VMEM((3,) + shape, f32),
                        dma((4,)), dma((4,)), dma((3,)), dma((3,)), dma((3,)), dma((3,)), dma((4,)), dma((4,))],
        compiler_params=pltpu.CompilerParams(collective_id=1, has_side_effects=True, vmem_limit_bytes=32 * 1024 * 1024),
        cost_estimate=pl.CostEstimate(flops=30_000_000_000, bytes_accessed=10_000_000, transcendentals=0),
        name='small_update',
    )(*lows, mom, var)


def local_step(tokens, d_logits, w_up, w_down, w_out, proj_up, proj_down, mom_up, var_up, mom_down, var_down, mom_out, var_out):
    num_layers = w_up.shape[0]
    hidden = tokens
    saved_acts = []
    for layer_idx in range(num_layers):
        pre_act = jnp.dot(hidden, w_up[layer_idx], preferred_element_type=jnp.float32).astype(jnp.bfloat16)
        post_act = gelu_tanh(pre_act.astype(jnp.float32)).astype(jnp.bfloat16)
        saved_acts.append((hidden, pre_act, post_act))
        hidden = (hidden.astype(jnp.float32) + jnp.dot(post_act, w_down[layer_idx], preferred_element_type=jnp.float32)).astype(jnp.bfloat16)

    devices = lax.axis_size(DATA_AXIS)
    mom_t, var_t = mom_out.T, var_out.T
    edge = lax.ppermute(jnp.stack([mom_t[:EDGE], var_t[:EDGE]]), DATA_AXIS, [(dev, dev - 1) for dev in range(1, devices)])
    left, right, m_raw, v_raw, grad_hidden = head_update(hidden, d_logits, w_out, mom_t, var_t, edge)
    far_x, far_y, far_xy, near = (1, 0, 0), (0, 1, 0), (1, 1, 0), (0, 0, 0)
    left_x = permute(left, far_x)
    right_y = permute(right, far_y)

    def with_core(pieces):
        return pieces + [(permute(piece, (0, 0, 1)), (far[0], far[1], 1), part) for piece, far, part in pieces]

    ups = []
    downs = []
    for layer_idx in reversed(range(num_layers)):
        hidden_in, pre_act, post_act = saved_acts[layer_idx]
        grad_down = jnp.einsum('tf,td->fd', post_act, grad_hidden, preferred_element_type=jnp.float32)
        d_post = jnp.einsum('td,fd->tf', grad_hidden, w_down[layer_idx], preferred_element_type=jnp.float32)
        gelu_pull = jax.vjp(gelu_tanh, pre_act.astype(jnp.float32))[1]
        d_pre = gelu_pull(d_post)[0].astype(jnp.bfloat16)
        if layer_idx == num_layers - 1:
            d_pre, left, right = lax.optimization_barrier((d_pre, left, right))
            left_y = permute(left, far_y)
            right_x = permute(right, far_x)
        else:
            d_pre = lax.optimization_barrier(d_pre)
        grad_up = jnp.einsum('tf,td->fd', d_pre, hidden_in, preferred_element_type=jnp.float32)
        if layer_idx > 0:
            grad_hidden = (grad_hidden.astype(jnp.float32) + jnp.einsum('tf,df->td', d_pre, w_up[layer_idx], preferred_element_type=jnp.float32)).astype(jnp.bfloat16)
        low_up = jnp.dot(grad_up, proj_up[layer_idx].astype(jnp.float32), preferred_element_type=jnp.float32)
        low_down = jnp.dot(grad_down, proj_down[layer_idx].astype(jnp.float32), preferred_element_type=jnp.float32)
        ups.append(low_up)
        downs.append(low_down)
    ups = ups[::-1]
    downs = downs[::-1]

    vocab = d_logits.shape[1]
    ups[0], downs[0], left_x, right_y = lax.optimization_barrier((ups[0], downs[0], left_x, right_y))
    left_xy = permute(left_x, far_y)
    right_xy = permute(right_y, far_x)
    own_pieces = with_core([(left, near, 0), (right, near, 1)])
    w_new, m_out, v_out = place(None, own_pieces, vocab, (m_raw, v_raw))
    w_new, = place(w_new, with_core([(left_x, far_x, 0), (right_y, far_y, 1)]), vocab)

    w_new, left_y, right_x = lax.optimization_barrier((w_new, left_y, right_x))
    w_new, = place(w_new, with_core([(left_y, far_y, 0), (right_x, far_x, 1)]), vocab)
    first = jnp.concatenate([jnp.swapaxes(mom_up, 1, 2), mom_down], axis=0)
    second = jnp.concatenate([jnp.swapaxes(var_up, 1, 2), var_down], axis=0)
    lows = ups + downs
    w_new, lows[0] = lax.optimization_barrier((w_new, lows[0]))
    m_low, v_low, dir_up, dir_down = small_update(lows, first, second)
    m_low, left_xy, right_xy = lax.optimization_barrier((m_low, left_xy, right_xy))
    step_up = jnp.einsum('ldr,lfr->ldf', proj_up, dir_up, preferred_element_type=jnp.float32)
    step_down = jnp.einsum('lfr,ldr->lfd', dir_down, proj_down, preferred_element_type=jnp.float32)
    w_up_new = (w_up.astype(jnp.float32) - LR * ALPHA * step_up).astype(jnp.bfloat16)
    w_down_new = (w_down.astype(jnp.float32) - LR * ALPHA * step_down).astype(jnp.bfloat16)

    w_out_new, = place(w_new, with_core([(left_xy, far_xy, 0), (right_xy, far_xy, 1)]), vocab)

    return (w_up_new, w_down_new, w_out_new,
            jnp.swapaxes(m_low[:num_layers], 1, 2), jnp.swapaxes(v_low[:num_layers], 1, 2),
            m_low[num_layers:], v_low[num_layers:],
            m_out.T, v_out.T)


def solution(mesh):
    row_spec = P(DATA_AXIS, None)
    whole = P()
    up_spec = P(None, None, DATA_AXIS)
    down_spec = P(None, DATA_AXIS, None)
    head_spec = P(None, DATA_AXIS)
    in_specs = (row_spec, row_spec, whole, whole, whole, whole, whole, up_spec, up_spec, down_spec, down_spec, head_spec, head_spec)
    out_specs = (whole, whole, whole, up_spec, up_spec, down_spec, down_spec, head_spec, head_spec)
    return jax.shard_map(local_step, mesh=mesh, in_specs=in_specs, out_specs=out_specs, check_vma=False)
```

```python
import functools

import jax
import jax.numpy as jnp
from jax import lax
from jax.experimental import pallas as pl
from jax.experimental.pallas import tpu as pltpu
from jax.sharding import PartitionSpec as P


BETA1 = 0.9
BETA2 = 0.999
EPS = 1e-8
STEP = 4
LR = 0.02
ALPHA = 0.5
LR_HEAD = 0.01
DATA_AXIS = 'data'
MESH = pl.DeviceIdType.MESH

BLK = 512
SUBS = 8
SHARD = 4000
RING = 5
EDGE = 96
DRING = 4

GROUP_DEST = (0, 1, 0, 1, 2, 0, 1, 2, 3, 0, 1, 2, 3, 2, 3, 3)
GROUP_PAIR = (0, 0, 1, 1, 0, 2, 2, 1, 0, 3, 3, 2, 1, 3, 2, 3)
GROUP_SEND = (0, 1, 2, 3, 4, 5, 6, 7, 0, 8, 9, 10, 0, 11, 0, 0)
BLOCKS = 64
LAG = 2
SLOTS = LAG + 2


def lookup(index, values):
    out = jnp.int32(values[-1])
    for position in range(len(values) - 1):
        out = jnp.where(index == position, jnp.int32(values[position]), out)
    return out


def gelu_tanh(values):
    return jax.nn.gelu(values, approximate=True)


def adam_update(gradient, moment_one, moment_two):
    moment_one = BETA1 * moment_one + (1.0 - BETA1) * gradient
    moment_two = BETA2 * moment_two + (1.0 - BETA2) * gradient * gradient
    direction = (moment_one / (1.0 - BETA1 ** STEP)) / (jnp.sqrt(moment_two / (1.0 - BETA2 ** STEP)) + EPS)
    return moment_one, moment_two, direction


def head_kernel(hidden, d_logits, w_out, mom, var, edge,
                w_left, w_right, mom_new, var_new, grad_hidden, recv_core, recv_first,
                hidden_t, dz_buf, wo_buf, acc, g_acc, add_core, add_first, recv_second, stage, moments, fin_w,
                dz_sem, wo_sem, core_sem, first_sem, second_sem, stage_sem, add_sem, load_sem, edge_sem, store_sem, fin_sem):
    me = lax.axis_index(DATA_AXIS)
    core = lax.rem(me, 2)
    pos_x = lax.rem(me // 2, 2)
    pos_y = me // 4
    partner = me + 1 - 2 * core
    near_x = me + 2 - 4 * pos_x
    near_y = me + 4 - 8 * pos_y

    def decode(n):
        group = n // 4
        half = lax.rem(n, 2)
        own = lax.rem(n // 2, 2)
        rel = lookup(group, GROUP_DEST)
        far_first = 1 - rel // 2
        far_second = 1 - lax.rem(rel, 2)
        sub = 2 * lookup(group, GROUP_PAIR) + half
        delta_x = jnp.where(half == 0, far_first, far_second)
        delta_y = jnp.where(half == 0, far_second, far_first)
        dest_x = pos_x + delta_x - 2 * pos_x * delta_x
        dest_y = pos_y + delta_y - 2 * pos_y * delta_y
        dest_core = jnp.where(own == 1, core, 1 - core)
        dest = (dest_y * 2 + dest_x) * 2 + dest_core
        col = pl.multiple_of(((125 * dest) // 4 + 4 * sub) * 128, 128)
        return group, half, own, rel, sub, dest, col

    def fetch(n):
        col = decode(n)[-1]
        slot = lax.rem(n, SLOTS)
        return (pltpu.make_async_copy(d_logits.at[:, pl.ds(col, BLK)], dz_buf.at[slot], dz_sem.at[slot]),
                pltpu.make_async_copy(w_out.at[:, pl.ds(col, BLK)], wo_buf.at[slot], wo_sem.at[slot]))

    def send(slot, target_ref, recv_sem, device):
        return pltpu.make_async_remote_copy(
            src_ref=stage.at[slot], dst_ref=target_ref, send_sem=stage_sem.at[slot], recv_sem=recv_sem,
            device_id=(device,), device_id_type=MESH)

    def to_core(slot, index):
        return send(slot, recv_core.at[index], core_sem.at[index], partner)

    def to_first(slot, index, device):
        return send(slot, recv_first.at[index], first_sem.at[index], device)

    def to_second(slot, index, device):
        return send(slot, recv_second.at[index], second_sem.at[index], device)

    def wait_slot(slot):
        to_core(slot, 0).wait_send()

    shift = 32 * lax.rem(me, 4)

    def moment_loads(sub, half):
        first_row = jnp.clip(BLK * sub - shift, 0, SHARD - BLK)
        place = pl.multiple_of(EDGE + first_row + shift - BLK * sub, 32)
        rows = pl.ds(pl.multiple_of(first_row, 32), BLK)
        return [pltpu.make_async_copy(source.at[rows], moments.at[half, kind, pl.ds(place, BLK)], load_sem.at[half, kind])
                for kind, source in enumerate((mom, var))]

    def edge_loads(half):
        place = pl.ds(pl.multiple_of(BLK + shift, 32), EDGE)
        return [pltpu.make_async_copy(edge.at[kind], moments.at[half, kind, place], edge_sem.at[half, kind])
                for kind in range(2)]

    def moment_stores(sub, half):
        pieces = [(None, EDGE, BLK - 2 * EDGE)]
        for step in range(3):
            pieces.append((jnp.logical_or(sub > 0, 32 * step >= shift), 32 * step, 32))
            pieces.append((jnp.logical_or(sub < SUBS - 1, 32 * step < shift), BLK - EDGE + 32 * step, 32))
        out = []
        for position, (needed, row, size) in enumerate(pieces):
            target = jnp.maximum(BLK * sub - shift + row, 0)
            rows = pl.ds(pl.multiple_of(target, 32), size)
            for kind, result in enumerate((mom_new, var_new)):
                out.append((needed, pltpu.make_async_copy(
                    moments.at[half, kind, pl.ds(EDGE + row, size)], result.at[rows], store_sem.at[half, kind, position])))
        return out

    def weight_stores(sub, half):
        cols = pl.ds(pl.multiple_of(lax.rem(sub, SUBS // 2) * BLK, BLK), BLK)
        return [(sub < SUBS // 2, pltpu.make_async_copy(fin_w.at[half], w_left.at[:, cols], fin_sem.at[half])),
                (sub >= SUBS // 2, pltpu.make_async_copy(fin_w.at[half], w_right.at[:, cols], fin_sem.at[half]))]

    def for_stores(sub, half, action):
        for needed, copy in moment_stores(sub, half) + weight_stores(sub, half):
            if needed is None:
                action(copy)
            else:
                pl.when(needed)(functools.partial(action, copy))

    for copy in fetch(jnp.int32(0)):
        copy.start()
    barrier = pltpu.get_barrier_semaphore()
    for other in (partner, near_x, near_y):
        pl.semaphore_signal(barrier, inc=1, device_id=(other,), device_id_type=MESH)

    @pl.loop(0, hidden.shape[0] // 512)
    def _(tile):
        rows = pl.ds(pl.multiple_of(tile * 512, 512), 512)
        hidden_t[:, rows] = hidden[rows, :].T

    g_acc[...] = jnp.zeros_like(g_acc)
    pl.semaphore_wait(barrier, 3)


    def body(n, carry):
        group, half, own, rel, sub, _, _ = decode(n)
        slot = lax.rem(n, SLOTS)

        @pl.when(n + 1 < BLOCKS)
        def _():
            for copy in fetch(n + 1):
                copy.start()

        core_index = sub * 4 + rel
        first_index = sub * 2 + 1 - lax.rem(rel, 2)
        needs_first = jnp.logical_and(own == 1, rel >= 2)
        is_final = jnp.logical_and(own == 1, rel == 3)
        load_core = pltpu.make_async_copy(recv_core.at[core_index], add_core.at[half], add_sem.at[half, 0])
        load_first = pltpu.make_async_copy(recv_first.at[first_index], add_first.at[half], add_sem.at[half, 1])

        @pl.when(own == 1)
        def _():
            to_core(0, core_index).wait_recv()
            load_core.start()

        @pl.when(needs_first)
        def _():
            to_first(0, first_index, near_x).wait_recv()
            load_first.start()

        for copy in fetch(n):
            copy.wait()

        @pl.loop(0, BLK // 256)
        def _(tile):
            cols = pl.ds(pl.multiple_of(tile * 256, 256), 256)
            acc[half, :, cols] = jnp.dot(hidden_t[...], dz_buf[slot, :, cols], preferred_element_type=jnp.float32)

        @pl.when(is_final)
        def _():
            @pl.when(sub >= 2)
            def _():
                for_stores(sub - 2, half, lambda copy: copy.wait())

            for copy in moment_loads(sub, half):
                copy.start()

            @pl.when(sub == SUBS - 1)
            def _():
                for copy in edge_loads(half):
                    copy.start()

            fin_w[half] = wo_buf[slot]

        @pl.when(own == 0)
        def _():
            place = 2 * RING + lax.rem(group, 2) * 2 + half

            @pl.when(group >= 2)
            def _():
                wait_slot(place)

            stage[place] = acc[half]
            to_core(place, core_index).start()

        turn = lookup(group, GROUP_SEND)
        along_y = jnp.where(rel < 2, half, 1 - half)
        place = along_y * RING + lax.rem(turn, RING)
        device = jnp.where(along_y == 1, near_y, near_x)

        @pl.when(jnp.logical_and(own == 1, rel < 2))
        def _():
            load_core.wait()

            @pl.when(turn >= RING)
            def _():
                wait_slot(place)

            stage[place] = acc[half] + add_core[half]
            to_first(place, first_index, device).start()

        @pl.when(jnp.logical_and(own == 1, rel == 2))
        def _():
            load_core.wait()
            load_first.wait()

            @pl.when(turn >= RING)
            def _():
                wait_slot(place)

            stage[place] = acc[half] + add_core[half] + add_first[half]
            to_second(place, sub, device).start()

        def hidden_part(block, carry):
            _, _, _, _, _, dest, col = decode(block)
            slot = lax.rem(block, SLOTS)
            lane = lax.broadcasted_iota(jnp.int32, (1, BLK), 1) + (col - SHARD * dest)
            keep = jnp.where(jnp.logical_and(lane >= 0, lane < SHARD), 1.0, 0.0).astype(jnp.bfloat16)
            weights = wo_buf[slot] * keep

            @pl.loop(0, 4)
            def _(tile):
                rows = pl.ds(pl.multiple_of(tile * 512, 512), 512)
                g_acc[rows, :] += lax.dot_general(dz_buf[slot, rows, :], weights, (((1,), (1,)), ((), ())),
                                                  preferred_element_type=jnp.float32)

            return carry

        last = n == BLOCKS - 1
        lax.fori_loop(jnp.maximum(n - LAG, 0), jnp.where(last, BLOCKS, jnp.maximum(n - LAG + 1, 0)), hidden_part, 0)

        @pl.when(jnp.logical_and(is_final, half == 1))
        def _():
            for part in range(2):
                this = sub - 1 + part
                to_second(0, this, near_x).wait_recv()
                pltpu.make_async_copy(recv_core.at[this * 4 + 3], add_core.at[part], add_sem.at[part, 0]).wait()
                pltpu.make_async_copy(recv_first.at[this * 2], add_first.at[part], add_sem.at[part, 1]).wait()
                for copy in moment_loads(this, part):
                    copy.wait()

                @pl.when(this == SUBS - 1)
                def _():
                    for copy in edge_loads(part):
                        copy.wait()

            @pl.loop(0, 2 * (BLK // 128))
            def _(tile):
                part = tile // (BLK // 128)
                tile = lax.rem(tile, BLK // 128)
                cols = pl.ds(pl.multiple_of(tile * 128, 128), 128)
                rows = pl.ds(pl.multiple_of(EDGE + tile * 128, 32), 128)
                total = acc[part, :, cols] + add_core[part, :, cols] + add_first[part, :, cols] + recv_second[sub - 1 + part, :, cols]
                first, second, direction = adam_update(total.T, moments[part, 0, rows, :], moments[part, 1, rows, :])
                moments[part, 0, rows, :] = first
                moments[part, 1, rows, :] = second
                fin_w[part, :, cols] = (fin_w[part, :, cols].astype(jnp.float32) - LR_HEAD * direction.T).astype(jnp.bfloat16)

            for part in range(2):
                for_stores(sub - 1 + part, part, lambda copy: copy.start())

        return carry

    lax.fori_loop(0, BLOCKS, body, 0)

    @pl.loop(0, 4)
    def _(tile):
        rows = pl.ds(pl.multiple_of(tile * 512, 512), 512)
        grad_hidden[rows, :] = g_acc[rows, :].astype(jnp.bfloat16)

    for half in range(2):
        for_stores(SUBS - 2 + half, half, lambda copy: copy.wait())
    for place in range(2 * RING + DRING):
        wait_slot(place)


def head_update(hidden, d_logits, w_out, mom_t, var_t, edge):
    tokens, dim = hidden.shape
    f32 = jnp.float32
    bf16 = jnp.bfloat16
    any_spec = pl.BlockSpec(memory_space=pl.ANY)
    vmem = pl.BlockSpec(memory_space=pltpu.VMEM)
    outs = pl.pallas_call(
        head_kernel,
        out_shape=(
            jax.ShapeDtypeStruct((dim, SUBS * BLK // 2), bf16),
            jax.ShapeDtypeStruct((dim, SUBS * BLK // 2), bf16),
            jax.ShapeDtypeStruct(mom_t.shape, f32),
            jax.ShapeDtypeStruct(var_t.shape, f32),
            pltpu.VMEM((tokens, dim), bf16),
            jax.ShapeDtypeStruct((4 * SUBS, dim, BLK), f32),
            jax.ShapeDtypeStruct((2 * SUBS, dim, BLK), f32),
        ),
        in_specs=[vmem] + [any_spec] * 5,
        out_specs=(any_spec, any_spec, any_spec, any_spec, vmem, any_spec, any_spec),
        scratch_shapes=[
            pltpu.VMEM((dim, tokens), bf16),
            pltpu.VMEM((SLOTS, tokens, BLK), bf16),
            pltpu.VMEM((SLOTS, dim, BLK), bf16),
            pltpu.VMEM((2, dim, BLK), f32),
            pltpu.VMEM((tokens, dim), f32),
            pltpu.VMEM((2, dim, BLK), f32),
            pltpu.VMEM((2, dim, BLK), f32),
            pltpu.VMEM((SUBS, dim, BLK), f32),
            pltpu.VMEM((2 * RING + DRING, dim, BLK), f32),
            pltpu.VMEM((2, 2, BLK + 2 * EDGE, dim), f32),
            pltpu.VMEM((2, dim, BLK), bf16),
            pltpu.SemaphoreType.DMA((SLOTS,)),
            pltpu.SemaphoreType.DMA((SLOTS,)),
            pltpu.SemaphoreType.DMA((4 * SUBS,)),
            pltpu.SemaphoreType.DMA((2 * SUBS,)),
            pltpu.SemaphoreType.DMA((SUBS,)),
            pltpu.SemaphoreType.DMA((2 * RING + DRING,)),
            pltpu.SemaphoreType.DMA((2, 2)),
            pltpu.SemaphoreType.DMA((2, 2)),
            pltpu.SemaphoreType.DMA((2, 2)),
            pltpu.SemaphoreType.DMA((2, 2, 7)),
            pltpu.SemaphoreType.DMA((2,)),
        ],
        compiler_params=pltpu.CompilerParams(collective_id=0, has_side_effects=True, vmem_limit_bytes=58 * 1024 * 1024),
        cost_estimate=pl.CostEstimate(flops=280_000_000_000, bytes_accessed=300_000_000, transcendentals=0),
        name='head_update',
    )(hidden, d_logits, w_out, mom_t, var_t, edge)
    return outs[:5]


def flip(me, far):
    for bit, weight in zip(far, (2, 4, 1)):
        if bit:
            me = me + weight - 2 * weight * lax.rem(me // weight, 2)
    return me


def permute(value, far):
    mask = 2 * far[0] + 4 * far[1] + far[2]
    return lax.ppermute(value, DATA_AXIS, [(dev, dev ^ mask) for dev in range(8)])


def place_kernel(origins, num_copies, has_base, *refs):
    count = len(origins)
    pieces = refs[:count]
    sources = refs[count:count + num_copies]
    refs = refs[count + num_copies + has_base:]
    out, targets = refs[0], refs[1:1 + num_copies]
    buf, in_sem, out_sem, edge_sem = refs[1 + num_copies:5 + num_copies]
    me = lax.axis_index(DATA_AXIS)
    width = pieces[0].shape[-1]
    loads = [pltpu.make_async_copy(piece, buf.at[position], in_sem.at[position]) for position, piece in enumerate(pieces)]
    for load in loads:
        load.start()
    if num_copies:
        wide, wide_in, wide_out = refs[5 + num_copies:]
        rows = wide.shape[1]
        steps = sources[0].shape[0] // rows
        work = [(kind, step) for step in range(steps) for kind in range(num_copies)]

        def wide_load(index):
            kind, step = work[index]
            return pltpu.make_async_copy(sources[kind].at[pl.ds(step * rows, rows)], wide.at[index % 4], wide_in.at[index % 4])

        def wide_store(index):
            kind, step = work[index]
            return pltpu.make_async_copy(wide.at[index % 4], targets[kind].at[pl.ds(step * rows, rows)], wide_out.at[index % 4])

        for index in range(2):
            wide_load(index).start()
        for index in range(len(work)):
            wide_load(index).wait()
            wide_store(index).start()
            if index + 2 < len(work):
                if index >= 2:
                    wide_store(index - 2).wait()
                wide_load(index + 2).start()
        for index in range(len(work) - 4, len(work)):
            wide_store(index).wait()
    stores = []
    for position, (far, part) in enumerate(origins):
        loads[position].wait()
        dest = flip(me, far)
        col = pl.multiple_of(((125 * dest) // 4) * 128 + part * width, 128)
        skip = 0 if part else 128
        store = pltpu.make_async_copy(buf.at[position, :, pl.ds(skip, width - skip)],
                                      out.at[:, pl.ds(pl.multiple_of(col + skip, 128), width - skip)], out_sem.at[position])
        store.start()
        stores.append(store)
        if not part:
            edge = pltpu.make_async_copy(buf.at[position, :, pl.ds(0, 128)], out.at[:, pl.ds(col, 128)], edge_sem.at[position])

            @pl.when(lax.rem(dest, 4) == 0)
            def _():
                edge.start()
                edge.wait()
    for store in stores:
        store.wait()


def place(base, placed, vocab, copies=()):
    pieces = [piece for piece, _, _ in placed]
    origins = tuple((far, part) for _, far, part in placed)
    dim, width = pieces[0].shape
    count = len(pieces)
    has_base = base is not None
    args = pieces + list(copies) + ([base] if has_base else [])
    scratch = [pltpu.VMEM((count, dim, width), jnp.bfloat16)] + [pltpu.SemaphoreType.DMA((count,))] * 3
    if copies:
        scratch += [pltpu.VMEM((4, 400, dim), jnp.float32), pltpu.SemaphoreType.DMA((4,)), pltpu.SemaphoreType.DMA((4,))]
    any_spec = pl.BlockSpec(memory_space=pl.ANY)
    outs = pl.pallas_call(
        functools.partial(place_kernel, origins, len(copies), int(has_base)),
        out_shape=[jax.ShapeDtypeStruct((dim, vocab), jnp.bfloat16)] + [jax.ShapeDtypeStruct(c.shape, c.dtype) for c in copies],
        in_specs=[any_spec] * len(args),
        out_specs=[any_spec] * (1 + len(copies)),
        scratch_shapes=scratch,
        input_output_aliases={len(args) - 1: 0} if has_base else {},
        compiler_params=pltpu.CompilerParams(vmem_limit_bytes=40 * 1024 * 1024),
        cost_estimate=pl.CostEstimate(flops=6_000_000_000 if copies else 3_000_000_000, bytes_accessed=count * 4 * dim * width, transcendentals=0),
        name='place',
    )(*args)
    return outs


NEAR = ((1, 0), (0, 1), (1, 1))


def small_kernel(up_0, up_1, down_0, down_1, mom, var, mom_new, var_new, dir_up, dir_down,
                 parts, dirs, whole, from_core, from_chip, stage,
                 core_send, core_recv, chip_send, chip_recv, gather_send, gather_recv, back_send, back_recv):
    me = lax.axis_index(DATA_AXIS)
    partner = flip(me, (0, 0, 1))
    chips = [me] + [flip(me, far + (0,)) for far in NEAR]
    barrier = pltpu.get_barrier_semaphore()
    for other in chips[1:] + [partner]:
        pl.semaphore_signal(barrier, inc=1, device_id=(other,), device_id_type=MESH)
    pl.semaphore_wait(barrier, 4)

    shard = parts.shape[2]
    lows = (up_0, up_1, down_0, down_1)
    for dev in range(parts.shape[0]):
        for kind, low in enumerate(lows):
            parts[dev, kind] = low[dev * shard:(dev + 1) * shard, :]

    def remote(source, target, send_sem, recv_sem, device):
        return pltpu.make_async_remote_copy(src_ref=source, dst_ref=target, send_sem=send_sem, recv_sem=recv_sem,
                                            device_id=(device,), device_id_type=MESH)

    order = (1, 2, 3, 0)
    to_core = {}
    for k in order:
        to_core[k] = remote(parts.at[flip(chips[k], (0, 0, 1))], from_core.at[k], core_send.at[k], core_recv.at[k], partner)
        to_core[k].start()
    to_chip = []
    for k in (1, 2, 3):
        to_core[k].wait_recv()
        stage[k - 1] = parts[chips[k]] + from_core[k]
        copy = remote(stage.at[k - 1], from_chip.at[k - 1], chip_send.at[k - 1], chip_recv.at[k - 1], chips[k])
        copy.start()
        to_chip.append(copy)
    to_core[0].wait_recv()
    for copy in to_chip:
        copy.wait_recv()
    total = parts[me] + from_core[0] + from_chip[0] + from_chip[1] + from_chip[2]
    first, second, direction = adam_update(total, mom[...], var[...])
    mom_new[...] = first
    var_new[...] = second
    dirs[me] = direction.astype(jnp.bfloat16)
    gather = [remote(dirs.at[me], dirs.at[me], gather_send.at[k - 1], gather_recv.at[k - 1], chips[k]) for k in (1, 2, 3)]
    back = [remote(dirs.at[chips[k]], dirs.at[chips[k]], back_send.at[k], back_recv.at[k], partner) for k in range(4)]
    for copy in gather:
        copy.start()
    back[0].start()
    for k in (1, 2, 3):
        remote(dirs.at[chips[k]], dirs.at[chips[k]], gather_send.at[k - 1], gather_recv.at[k - 1], chips[k]).wait_recv()
        back[k].start()
    for k in range(4):
        remote(dirs.at[flip(chips[k], (0, 0, 1))], dirs.at[flip(chips[k], (0, 0, 1))], back_send.at[k], back_recv.at[k], partner).wait_recv()
        back[k].wait_send()
        to_core[k].wait_send()
    for copy in gather + to_chip:
        copy.wait_send()
    for kind in range(4):
        for dev in range(parts.shape[0]):
            whole[dev * shard:(dev + 1) * shard, :] = dirs[dev, kind].astype(jnp.float32)
        target = dir_up if kind < 2 else dir_down
        target[kind % 2] = whole[...].astype(jnp.bfloat16)


def small_update(lows, mom, var):
    shape = mom.shape
    rows, rank = lows[0].shape
    devices = rows // shape[1]
    f32 = jnp.float32
    vmem = pl.BlockSpec(memory_space=pltpu.VMEM)
    dma = pltpu.SemaphoreType.DMA
    return pl.pallas_call(
        small_kernel,
        out_shape=(jax.ShapeDtypeStruct(shape, f32), jax.ShapeDtypeStruct(shape, f32),
                   jax.ShapeDtypeStruct((2, rows, rank), jnp.bfloat16), jax.ShapeDtypeStruct((2, rows, rank), jnp.bfloat16)),
        in_specs=[vmem] * 6,
        out_specs=(vmem,) * 4,
        scratch_shapes=[pltpu.VMEM((devices,) + shape, f32), pltpu.VMEM((devices,) + shape, jnp.bfloat16),
                        pltpu.VMEM((rows, rank), f32), pltpu.VMEM((4,) + shape, f32), pltpu.VMEM((3,) + shape, f32), pltpu.VMEM((3,) + shape, f32),
                        dma((4,)), dma((4,)), dma((3,)), dma((3,)), dma((3,)), dma((3,)), dma((4,)), dma((4,))],
        compiler_params=pltpu.CompilerParams(collective_id=1, has_side_effects=True, vmem_limit_bytes=32 * 1024 * 1024),
        cost_estimate=pl.CostEstimate(flops=30_000_000_000, bytes_accessed=10_000_000, transcendentals=0),
        name='small_update',
    )(*lows, mom, var)


def local_step(tokens, d_logits, w_up, w_down, w_out, proj_up, proj_down, mom_up, var_up, mom_down, var_down, mom_out, var_out):
    num_layers = w_up.shape[0]
    hidden = tokens
    saved_acts = []
    for layer_idx in range(num_layers):
        pre_act = jnp.dot(hidden, w_up[layer_idx], preferred_element_type=jnp.float32).astype(jnp.bfloat16)
        post_act = gelu_tanh(pre_act.astype(jnp.float32)).astype(jnp.bfloat16)
        saved_acts.append((hidden, pre_act, post_act))
        hidden = (hidden.astype(jnp.float32) + jnp.dot(post_act, w_down[layer_idx], preferred_element_type=jnp.float32)).astype(jnp.bfloat16)

    devices = lax.axis_size(DATA_AXIS)
    mom_t, var_t = mom_out.T, var_out.T
    edge = lax.ppermute(jnp.stack([mom_t[:EDGE], var_t[:EDGE]]), DATA_AXIS, [(dev, dev - 1) for dev in range(1, devices)])
    left, right, m_raw, v_raw, grad_hidden = head_update(hidden, d_logits, w_out, mom_t, var_t, edge)
    far_x, far_y, far_xy, near = (1, 0, 0), (0, 1, 0), (1, 1, 0), (0, 0, 0)
    left_x = permute(left, far_x)
    right_y = permute(right, far_y)

    def with_core(pieces):
        return pieces + [(permute(piece, (0, 0, 1)), (far[0], far[1], 1), part) for piece, far, part in pieces]

    ups = []
    downs = []
    for layer_idx in reversed(range(num_layers)):
        hidden_in, pre_act, post_act = saved_acts[layer_idx]
        grad_down = jnp.einsum('tf,td->fd', post_act, grad_hidden, preferred_element_type=jnp.float32)
        d_post = jnp.einsum('td,fd->tf', grad_hidden, w_down[layer_idx], preferred_element_type=jnp.float32)
        gelu_pull = jax.vjp(gelu_tanh, pre_act.astype(jnp.float32))[1]
        d_pre = gelu_pull(d_post)[0].astype(jnp.bfloat16)
        if layer_idx == num_layers - 1:
            d_pre, left, right = lax.optimization_barrier((d_pre, left, right))
            left_y = permute(left, far_y)
            right_x = permute(right, far_x)
        else:
            d_pre = lax.optimization_barrier(d_pre)
        grad_up = jnp.einsum('tf,td->fd', d_pre, hidden_in, preferred_element_type=jnp.float32)
        if layer_idx > 0:
            grad_hidden = (grad_hidden.astype(jnp.float32) + jnp.einsum('tf,df->td', d_pre, w_up[layer_idx], preferred_element_type=jnp.float32)).astype(jnp.bfloat16)
        low_up = jnp.dot(grad_up, proj_up[layer_idx].astype(jnp.float32), preferred_element_type=jnp.float32)
        low_down = jnp.dot(grad_down, proj_down[layer_idx].astype(jnp.float32), preferred_element_type=jnp.float32)
        ups.append(low_up)
        downs.append(low_down)
    ups = ups[::-1]
    downs = downs[::-1]

    vocab = d_logits.shape[1]
    ups[0], downs[0], left_x, right_y = lax.optimization_barrier((ups[0], downs[0], left_x, right_y))
    left_xy = permute(left_x, far_y)
    right_xy = permute(right_y, far_x)
    own_pieces = with_core([(left, near, 0), (right, near, 1)])
    w_new, m_out, v_out = place(None, own_pieces, vocab, (m_raw, v_raw))
    w_new, = place(w_new, with_core([(left_x, far_x, 0), (right_y, far_y, 1)]), vocab)

    w_new, left_y, right_x = lax.optimization_barrier((w_new, left_y, right_x))
    w_new, = place(w_new, with_core([(left_y, far_y, 0), (right_x, far_x, 1)]), vocab)
    first = jnp.concatenate([jnp.swapaxes(mom_up, 1, 2), mom_down], axis=0)
    second = jnp.concatenate([jnp.swapaxes(var_up, 1, 2), var_down], axis=0)
    lows = ups + downs
    w_new, lows[0] = lax.optimization_barrier((w_new, lows[0]))
    m_low, v_low, dir_up, dir_down = small_update(lows, first, second)
    m_low, left_xy, right_xy = lax.optimization_barrier((m_low, left_xy, right_xy))
    step_up = jnp.einsum('ldr,lfr->ldf', proj_up, dir_up, preferred_element_type=jnp.float32)
    step_down = jnp.einsum('lfr,ldr->lfd', dir_down, proj_down, preferred_element_type=jnp.float32)
    w_up_new = (w_up.astype(jnp.float32) - LR * ALPHA * step_up).astype(jnp.bfloat16)
    w_down_new = (w_down.astype(jnp.float32) - LR * ALPHA * step_down).astype(jnp.bfloat16)

    w_out_new, = place(w_new, with_core([(left_xy, far_xy, 0), (right_xy, far_xy, 1)]), vocab)

    return (w_up_new, w_down_new, w_out_new,
            jnp.swapaxes(m_low[:num_layers], 1, 2), jnp.swapaxes(v_low[:num_layers], 1, 2),
            m_low[num_layers:], v_low[num_layers:],
            m_out.T, v_out.T)


def solution(mesh):
    row_spec = P(DATA_AXIS, None)
    whole = P()
    up_spec = P(None, None, DATA_AXIS)
    down_spec = P(None, DATA_AXIS, None)
    head_spec = P(None, DATA_AXIS)
    in_specs = (row_spec, row_spec, whole, whole, whole, whole, whole, up_spec, up_spec, down_spec, down_spec, head_spec, head_spec)
    out_specs = (whole, whole, whole, up_spec, up_spec, down_spec, down_spec, head_spec, head_spec)
    return jax.shard_map(local_step, mesh=mesh, in_specs=in_specs, out_specs=out_specs, check_vma=False)
```
